32 devices in a mesh: dp: 4 (over y, z), cp: 8 (over x, core).
Axes of the slice: x: 4, y: 2, z: 2, core: 2. Of those that a mesh axis runs over, the one named last changes fastest.
The devices are a block of a 4x4x8 slice.
Arguments:
- query: bfloat16 [32, 512, 16, 128], P('dp', 'cp'), parts along dimension 0
- keys: bfloat16 [32, 512, 1, 128], P('dp', 'cp'), parts along dimension 0
- values: bfloat16 [32, 512, 1, 128], P('dp', 'cp'), parts along dimension 0
- grad_out: bfloat16 [32, 512, 16, 128], P('dp', 'cp'), parts along dimension 0
- doc_id: int32 [32, 512], P('dp', 'cp'), parts along dimension 0
Outputs:
- output 1: bfloat16 [32, 512, 16, 128], P('dp', 'cp'), parts along dimension 0
- output 2: bfloat16 [32, 512, 16, 128], P('dp', 'cp'), parts along dimension 0
- output 3: bfloat16 [32, 512, 1, 128], P('dp', 'cp'), parts along dimension 0
- output 4: bfloat16 [32, 512, 1, 128], P('dp', 'cp'), parts along dimension 0
There are 4 independent parts. The reference program is written for one: setup_inputs(seed, part) draws one part's arguments, and reference() takes and returns one part's arrays. A program takes and returns all parts, laid end to end along the dimension named above; each array names one.
All inputs are finite; a program needn't handle non-finite values.
Results may differ from the reference program's by a relative error of at most 0.0111373.
Values are sent between devices in bfloat16 or wider.
A program may use at most 768 MiB of HBM per device.

```python
import jax
import jax.numpy as jnp
from jax import lax

BATCH = 8
SEQ = 512
HEADS = 16
HEAD = 128
ROW_BLOCK = 8
DOC_CUTS = 4
NEG_BIG = -1e30


def doc_ids_row(key):
    key_cut, key_count = jax.random.split(key)
    cut_pos = jax.random.permutation(key_cut, SEQ - 1)[:DOC_CUTS] + 1
    cut_count = jax.random.randint(key_count, (), 1, DOC_CUTS + 1)
    cut_valid = jnp.arange(DOC_CUTS) < cut_count
    positions = jnp.arange(SEQ)
    cut_hits = (cut_pos[None, :] <= positions[:, None]) & cut_valid[None, :]
    return jnp.sum(cut_hits.astype(jnp.int32), axis=1).astype(jnp.int32)


def setup_inputs(seed: int = 0, part: int = 0) -> dict:
    key = jax.random.fold_in(jax.random.key(seed), part)
    key_q, key_k, key_v, key_slow, key_g, key_doc = jax.random.split(key, 6)
    query = 1.5 * jax.random.normal(key_q, (BATCH, SEQ, HEADS, HEAD), jnp.float32)
    keys = 1.5 * jax.random.normal(key_k, (BATCH, SEQ, 1, HEAD), jnp.float32)
    slow = jax.random.normal(key_slow, (BATCH, 16, 1, HEAD), jnp.float32)
    noise = jax.random.normal(key_v, (BATCH, SEQ, 1, HEAD), jnp.float32)
    values = 0.8 * jnp.repeat(slow, SEQ // 16, axis=1) + 0.6 * noise
    grad_out = 0.5 * jax.random.normal(key_g, (BATCH, SEQ, HEADS, HEAD), jnp.float32)
    doc_id = jax.vmap(doc_ids_row)(jax.random.split(key_doc, BATCH))
    return {'query': query.astype(jnp.bfloat16), 'keys': keys.astype(jnp.bfloat16), 'values': values.astype(jnp.bfloat16), 'grad_out': grad_out.astype(jnp.bfloat16), 'doc_id': doc_id}


def reference(query, keys, values, grad_out, doc_id):
    score_scale = HEAD ** -0.5
    n_blocks = SEQ // ROW_BLOCK
    key_pos = jnp.arange(SEQ)
    pos_blocks = key_pos.reshape(n_blocks, ROW_BLOCK)

    def one_row(row):
        q_row, k_row, v_row, g_row, doc_row = row
        k_mat = k_row[:, 0, :].astype(jnp.float32)
        v_mat = v_row[:, 0, :].astype(jnp.float32)
        q_blocks = q_row.reshape(n_blocks, ROW_BLOCK, HEADS, HEAD)
        g_blocks = g_row.reshape(n_blocks, ROW_BLOCK, HEADS, HEAD)
        doc_blocks = doc_row.reshape(n_blocks, ROW_BLOCK)

        def step(carry, block):
            dk_acc, dv_acc = carry
            q_block, g_block, doc_block, pos_block = block
            q_wide = q_block.astype(jnp.float32)
            g_wide = g_block.astype(jnp.float32)
            visible = (key_pos[None, :] <= pos_block[:, None]) & (doc_row[None, :] == doc_block[:, None])
            raw_scores = jnp.einsum('qhd,kd->qhk', q_wide, k_mat) * score_scale
            scores = jnp.where(visible[:, None, :], raw_scores, NEG_BIG)
            exp_scores = jnp.exp(scores - jnp.max(scores, axis=-1, keepdims=True))
            prob_f32 = exp_scores / jnp.sum(exp_scores, axis=-1, keepdims=True)
            prob_low = prob_f32.astype(jnp.bfloat16).astype(jnp.float32)
            out_block = jnp.einsum('qhk,kd->qhd', prob_low, v_mat).astype(jnp.bfloat16)
            row_delta = jnp.einsum('qhd,qhd->qh', g_wide, out_block.astype(jnp.float32))
            grad_prob = jnp.einsum('qhd,kd->qhk', g_wide, v_mat)
            grad_score = (prob_f32 * (grad_prob - row_delta[:, :, None])).astype(jnp.bfloat16).astype(jnp.float32)
            dq_block = (jnp.einsum('qhk,kd->qhd', grad_score, k_mat) * score_scale).astype(jnp.bfloat16)
            dk_acc = dk_acc + jnp.einsum('qhk,qhd->kd', grad_score, q_wide)
            dv_acc = dv_acc + jnp.einsum('qhk,qhd->kd', prob_low, g_wide)
            return (dk_acc, dv_acc), (out_block, dq_block)

        kv_zero = jnp.zeros((SEQ, HEAD), jnp.float32)
        sums, blocks = lax.scan(step, (kv_zero, kv_zero), (q_blocks, g_blocks, doc_blocks, pos_blocks))
        out_row = blocks[0].reshape(SEQ, HEADS, HEAD)
        dq_row = blocks[1].reshape(SEQ, HEADS, HEAD)
        dk_row = (sums[0] * score_scale).astype(jnp.bfloat16)[:, None, :]
        dv_row = sums[1].astype(jnp.bfloat16)[:, None, :]
        return out_row, dq_row, dk_row, dv_row

    attn_out, grad_query, grad_keys, grad_values = lax.map(one_row, (query, keys, values, grad_out, doc_id))
    return (attn_out, grad_query, grad_keys, grad_values)
```

```python
import functools
import math

import jax
import jax.numpy as jnp
from jax import lax
from jax.experimental import pallas as pl
from jax.experimental.pallas import tpu as pltpu
from jax.sharding import PartitionSpec as P

NEG_BIG = -1e30
POS_BIG = 3e38
MESH = pl.DeviceIdType.MESH
NT = (((1,), (1,)), ((), ()))
TN = (((0,), (0,)), ((), ()))
CORES = 2
ROWS = 256
LANE = 128


def dot(a, b, dims=(((1,), (0,)), ((), ()))):
    return lax.dot_general(a, b, dims, preferred_element_type=jnp.float32)


def kernel(n_grp, heads,
           q_in, g_in, k_in, v_in, doc_in,
           o_out, dq_out, dk_out, dv_out,
           q_v, g_v, o_v, dq_v, kv, doc_own, docs, key_doc, qry_doc, cap,
           part, peer_part, comb, far_part, fin, peer_fin,
           in_sem, qg_sem, doc_send, doc_recv, kv_send, kv_recv, fwd_send,
           pp_send, pp_recv, far_send, far_recv, fin_send, fin_recv, out_sem):
    n_batch, n_rows, dim = q_v.shape
    piece = n_rows // heads
    n_keys = n_grp * piece
    n_chip = n_grp // CORES
    scale = dim ** -0.5
    rank = lax.axis_index('cp')
    chip = rank // CORES
    core = rank % CORES
    peer = chip * CORES + (1 - core)

    def at(p):
        return pl.ds(pl.multiple_of(p * piece, piece), piece)

    def remote(src, dst, send, recv, to):
        return pltpu.make_async_remote_copy(
            src_ref=src, dst_ref=dst, send_sem=send, recv_sem=recv,
            device_id={'cp': to}, device_id_type=MESH)

    own_k = pltpu.make_async_copy(k_in, kv.at[:, 0, at(rank), :], in_sem.at[0])
    own_v = pltpu.make_async_copy(v_in, kv.at[:, 1, at(rank), :], in_sem.at[1])
    own_d = pltpu.make_async_copy(doc_in, doc_own, in_sem.at[2])
    own_k.start()
    own_v.start()
    own_d.start()

    def q_copy(b):
        return pltpu.make_async_copy(q_in.at[b], q_v.at[b], qg_sem.at[b, 0])

    def g_copy(b):
        return pltpu.make_async_copy(g_in.at[b], g_v.at[b], qg_sem.at[b, 1])

    for b in range(n_batch):
        q_copy(b).start()
        g_copy(b).start()

    barrier = pltpu.get_barrier_semaphore()
    for step in range(1, n_grp):
        pl.semaphore_signal(barrier, inc=1, device_id={'cp': (rank + step) % n_grp},
                            device_id_type=MESH)

    def clear(p, _):
        kv[:, 0, at(p), :] = jnp.zeros((n_batch, piece, dim), kv.dtype)
        kv[:, 1, at(p), :] = jnp.zeros((n_batch, piece, dim), kv.dtype)
        docs[p] = jnp.zeros(docs.shape[1:], docs.dtype)
        return 0

    lax.fori_loop(rank + 1, n_grp, clear, 0)
    own_d.wait()
    own = doc_own[...]
    wide = jnp.concatenate([own, own], axis=1)
    lane = lax.broadcasted_iota(jnp.int32, wide.shape, 1)
    docs[rank] = jnp.where(lane // piece == core, wide, 0)
    own_k.wait()
    own_v.wait()
    pl.semaphore_wait(barrier, n_grp - 1)

    def doc_copy(to):
        return remote(docs.at[rank], docs.at[rank], doc_send.at[to], doc_recv.at[rank], to)

    def kv_copy(b, to):
        src = kv.at[b, :, at(rank), :]
        return remote(src, src, kv_send.at[b, to // CORES], kv_recv.at[b, rank], to)

    def fwd_copy(b, src_chip):
        p = src_chip * CORES + core
        src = kv.at[b, :, at(p), :]
        return remote(src, src, fwd_send.at[b, src_chip], kv_recv.at[b, p], peer)

    for to in range(n_grp):
        @pl.when(to > rank)
        def _():
            doc_copy(to).start()

    def send_own(b, _):
        @pl.when(core == 0)
        def _():
            kv_copy(b, peer).start()
        for far in range(n_chip - 1, 0, -1):
            @pl.when(far > chip)
            def _():
                kv_copy(b, far * CORES + core).start()
        return 0

    lax.fori_loop(0, n_batch, send_own, 0)

    def kv_arrival(b, p):
        src = kv.at[b, :, at(p), :]
        return remote(src, src, kv_send.at[b, 0], kv_recv.at[b, p], peer)

    def forward(b):
        for src_chip in range(n_chip - 1):
            @pl.when(src_chip < chip)
            def _():
                kv_arrival(b, src_chip * CORES + core).wait_recv()
                fwd_copy(b, src_chip).start()

    def arrived(b):
        for src_chip in range(n_chip - 1):
            @pl.when(src_chip < chip)
            def _():
                kv_arrival(b, src_chip * CORES + 1 - core).wait_recv()

        @pl.when(core == 1)
        def _():
            kv_arrival(b, chip * CORES).wait_recv()

    own_t = wide.T
    for b in range(n_batch):
        qry_doc[b] = jnp.broadcast_to(own_t[:piece, b:b + 1], (piece, LANE))
    forward(0)
    for p in range(n_grp):
        @pl.when(p < rank)
        def _():
            remote(docs.at[p], docs.at[p], doc_send.at[p], doc_recv.at[p], peer).wait_recv()
    for t in range(n_chip):
        ids = docs[CORES * t] + docs[CORES * t + 1]
        for b in range(n_batch):
            key_doc[b, :, t * LANE:(t + 1) * LANE] = ids[b:b + 1]

    def pp_copy(b, t):
        return remote(part.at[b, 1 - core, t], peer_part.at[b, t], pp_send.at[b, t],
                      pp_recv.at[b, t], peer)

    def far_copy(b, t):
        slot = chip - t - 1
        return remote(comb.at[b, t], far_part.at[b, slot], far_send.at[b, t],
                      far_recv.at[b, slot], t * CORES + core)

    def tiles(fn):
        for t in range(n_chip):
            @pl.when(t <= chip)
            def _():
                fn(t)

    def combine(b):
        def one(t):
            pp_copy(b, t).wait_recv()
            comb[b, t] = part[b, core, t] + peer_part[b, t]
        tiles(one)

    def send_far(b):
        for t in range(n_chip):
            @pl.when(t < chip)
            def _():
                far_copy(b, t).start()

    def block(b, i, keys):
        rows = pl.ds(i * ROWS, ROWS)
        toks = ROWS // heads
        q = q_v[b, rows, :]
        g = g_v[b, rows, :]
        k = kv[b, 0, 0:keys, :]
        v = kv[b, 1, 0:keys, :]
        s = dot(q, k, NT)
        lim = cap[i * toks:(i + 1) * toks, 0:keys]
        lim = jnp.broadcast_to(lim[:, None, :], (toks, heads, keys)).reshape(ROWS, keys)
        s = jnp.minimum(s, lim)
        top = jnp.max(s, axis=-1, keepdims=True)
        e = jnp.exp2((s - top) * (scale * math.log2(math.e)))
        prob = e * (1.0 / jnp.sum(e, axis=-1, keepdims=True))
        prob_low = prob.astype(jnp.bfloat16)
        o = dot(prob_low, v).astype(jnp.bfloat16)
        o_v[b, rows, :] = o
        delta = jnp.sum(g.astype(jnp.float32) * o.astype(jnp.float32), axis=-1, keepdims=True)
        dp = dot(g, v, NT)
        ds = (prob * (dp - delta)).astype(jnp.bfloat16)
        dq_v[b, rows, :] = (dot(ds, k) * scale).astype(jnp.bfloat16)
        dk = dot(q, ds, TN)
        dv = dot(g, prob_low, TN)
        for t in range(keys // LANE):
            cols = slice(t * LANE, (t + 1) * LANE)
            if i == 0:
                part[b, 0, t] = dk[:, cols]
                part[b, 1, t] = dv[:, cols]
            else:
                part[b, 0, t] += dk[:, cols]
                part[b, 1, t] += dv[:, cols]

    def compute(b, first, last, keys):
        for i in range(first, last):
            block(b, i, keys)

    n_blocks = n_rows // ROWS
    half = n_keys // 2

    def compute_for_chip(b, first, last):
        @pl.when(chip < n_chip // 2)
        def _():
            compute(b, first, last, half)

        @pl.when(chip >= n_chip // 2)
        def _():
            compute(b, first, last, n_keys)

    def out_copies(b):
        return (pltpu.make_async_copy(o_v.at[b], o_out.at[b], out_sem.at[b, 0]),
                pltpu.make_async_copy(dq_v.at[b], dq_out.at[b], out_sem.at[b, 1]))

    def step(b, _):
        q_copy(b).wait()
        g_copy(b).wait()
        arrived(b)
        q_pos = rank * piece + lax.broadcasted_iota(jnp.int32, (piece, LANE), 0)
        for t in range(n_chip):
            k_pos = t * LANE + lax.broadcasted_iota(jnp.int32, (piece, LANE), 1)
            ids = jnp.broadcast_to(key_doc[b, :, t * LANE:(t + 1) * LANE], (piece, LANE))
            seen = (ids == qry_doc[b]) & (k_pos <= q_pos)
            cap[:, t * LANE:(t + 1) * LANE] = jnp.where(seen, POS_BIG, NEG_BIG)
        compute_for_chip(b, 0, n_blocks // 2)

        @pl.when(b > 0)
        def _():
            combine(b - 1)

        @pl.when(b + 1 < n_batch)
        def _():
            forward(b + 1)

        @pl.when(b > 0)
        def _():
            send_far(b - 1)
        compute_for_chip(b, n_blocks // 2, n_blocks)
        tiles(lambda t: pp_copy(b, t).start())
        for copy in out_copies(b):
            copy.start()
        return 0

    lax.fori_loop(0, n_batch, step, 0)
    combine(n_batch - 1)
    send_far(n_batch - 1)

    def fin_copy(b):
        return remote(fin.at[b, at(1 - core), :], peer_fin.at[b], fin_send.at[b],
                      fin_recv.at[b], peer)

    unit = jnp.where(core == 0, jnp.float32(scale), jnp.float32(1.0))

    def finish(b, _):
        fin_acc = comb[b, chip]
        peer_part[b, 0] = fin_acc
        for slot in range(n_chip - 1):
            @pl.when(slot < n_chip - 1 - chip)
            def _():
                remote(comb.at[b, 0], far_part.at[b, slot], far_send.at[b, 0],
                       far_recv.at[b, slot], peer).wait_recv()
                peer_part[b, 0] += far_part[b, slot]
        fin[b] = (peer_part[b, 0].T * unit).astype(jnp.bfloat16)
        fin_copy(b).start()
        return 0

    lax.fori_loop(0, n_batch, finish, 0)

    def settle(b, _):
        fin_copy(b).wait_recv()
        return 0

    lax.fori_loop(0, n_batch, settle, 0)

    mine = fin.at[:, at(core), :]
    for this in range(CORES):
        @pl.when(core == this)
        def _():
            ours, theirs = (dk_out, dv_out) if this == 0 else (dv_out, dk_out)
            copies = (pltpu.make_async_copy(mine, ours, in_sem.at[0]),
                      pltpu.make_async_copy(peer_fin, theirs, in_sem.at[1]))
            for copy in copies:
                copy.start()
            for copy in copies:
                copy.wait()

    for to in range(n_grp):
        @pl.when(to > rank)
        def _():
            doc_copy(to).wait_send()

    def drain(b, _):
        @pl.when(core == 0)
        def _():
            kv_copy(b, peer).wait_send()
        for far in range(1, n_chip):
            @pl.when(far > chip)
            def _():
                kv_copy(b, far * CORES + core).wait_send()
        for t in range(n_chip):
            @pl.when(t < chip)
            def _():
                fwd_copy(b, t).wait_send()
                far_copy(b, t).wait_send()
        tiles(lambda t: pp_copy(b, t).wait_send())
        fin_copy(b).wait_send()
        for copy in out_copies(b):
            copy.wait()
        return 0

    lax.fori_loop(0, n_batch, drain, 0)


def solution(mesh):
    n_grp = mesh.shape['cp']
    n_chip = n_grp // CORES
    seq_spec = P('dp', 'cp', None, None)
    id_spec = P('dp', 'cp')

    def per_device(query, keys, values, grad_out, doc_id):
        n_batch, piece, heads, dim = query.shape
        n_rows = piece * heads
        n_keys = n_grp * piece
        flat = (n_batch, n_rows, dim)
        small = (n_batch, piece, dim)
        bf16, f32, i32 = jnp.bfloat16, jnp.float32, jnp.int32
        any_spec = pl.BlockSpec(memory_space=pl.ANY)
        dma = pltpu.SemaphoreType.DMA
        tile = (dim, LANE)
        outs = pl.pallas_call(
            functools.partial(kernel, n_grp, heads),
            out_shape=[jax.ShapeDtypeStruct(flat, bf16), jax.ShapeDtypeStruct(flat, bf16),
                       jax.ShapeDtypeStruct(small, bf16), jax.ShapeDtypeStruct(small, bf16)],
            in_specs=[any_spec] * 5,
            out_specs=[any_spec] * 4,
            scratch_shapes=[
                pltpu.VMEM(flat, bf16), pltpu.VMEM(flat, bf16),
                pltpu.VMEM(flat, bf16), pltpu.VMEM(flat, bf16),
                pltpu.VMEM((n_batch, 2, n_keys, dim), bf16),
                pltpu.VMEM((n_batch, piece), i32),
                pltpu.VMEM((n_grp, n_batch, LANE), i32),
                pltpu.VMEM((n_batch, 1, n_keys), i32),
                pltpu.VMEM((n_batch, piece, LANE), i32),
                pltpu.VMEM((piece, n_keys), f32),
                pltpu.VMEM((n_batch, 2, n_chip) + tile, f32),
                pltpu.VMEM((n_batch, n_chip) + tile, f32),
                pltpu.VMEM((n_batch, n_chip) + tile, f32),
                pltpu.VMEM((n_batch, n_chip - 1) + tile, f32),
                pltpu.VMEM((n_batch, LANE, dim), bf16),
                pltpu.VMEM(small, bf16),
                dma((3,)), dma((n_batch, 2)), dma((n_grp,)), dma((n_grp,)),
                dma((n_batch, n_chip)), dma((n_batch, n_grp)), dma((n_batch, n_chip)),
                dma((n_batch, n_chip)), dma((n_batch, n_chip)),
                dma((n_batch, n_chip)), dma((n_batch, n_chip)),
                dma((n_batch,)), dma((n_batch,)), dma((n_batch, 2)),
            ],
            compiler_params=pltpu.CompilerParams(
                collective_id=0, has_side_effects=True, vmem_limit_bytes=48 * 2**20),
            name='mqa',
        )(query.reshape(flat), grad_out.reshape(flat), keys.reshape(small),
          values.reshape(small), doc_id)
        attn_out, grad_query, grad_keys, grad_values = outs
        return (attn_out.reshape(query.shape), grad_query.reshape(query.shape),
                grad_keys.reshape(keys.shape), grad_values.reshape(values.shape))

    return jax.shard_map(per_device, mesh=mesh,
                         in_specs=(seq_spec, seq_spec, seq_spec, seq_spec, id_spec),
                         out_specs=(seq_spec, seq_spec, seq_spec, seq_spec), check_vma=False)
```

```python
import functools
import math

import jax
import jax.numpy as jnp
from jax import lax
from jax.experimental import pallas as pl
from jax.experimental.pallas import tpu as pltpu
from jax.sharding import PartitionSpec as P

NEG_BIG = -1e30
POS_BIG = 3e38
MESH = pl.DeviceIdType.MESH
NT = (((1,), (1,)), ((), ()))
TN = (((0,), (0,)), ((), ()))
CORES = 2
ROWS = 512
AHEAD = 2
LANE = 128


def dot(a, b, dims=(((1,), (0,)), ((), ()))):
    return lax.dot_general(a, b, dims, preferred_element_type=jnp.float32)


def kernel(n_grp, heads,
           q_in, g_in, k_in, v_in, doc_in,
           o_out, dq_out, dk_out, dv_out,
           q_v, g_v, o_v, dq_v, kv, doc_own, docs, key_doc, qry_doc, cap, p_low, d_low,
           part, peer_part, comb, far_part, fin, peer_fin,
           in_sem, qg_sem, doc_send, doc_recv, kv_send, kv_recv, fwd_send, fwd_recv,
           pp_send, pp_recv, far_send, far_recv, fin_send, fin_recv, out_sem):
    n_batch, n_rows, dim = q_v.shape
    piece = n_rows // heads
    n_keys = n_grp * piece
    n_chip = n_grp // CORES
    scale = dim ** -0.5
    rank = lax.axis_index('cp')
    chip = rank // CORES
    core = rank % CORES
    peer = chip * CORES + (1 - core)

    def at(p):
        return pl.ds(pl.multiple_of(p * piece, piece), piece)

    def remote(src, dst, send, recv, to):
        return pltpu.make_async_remote_copy(
            src_ref=src, dst_ref=dst, send_sem=send, recv_sem=recv,
            device_id={'cp': to}, device_id_type=MESH)

    own_k = pltpu.make_async_copy(k_in, kv.at[:, 0, at(rank), :], in_sem.at[0])
    own_v = pltpu.make_async_copy(v_in, kv.at[:, 1, at(rank), :], in_sem.at[1])
    own_d = pltpu.make_async_copy(doc_in, doc_own, in_sem.at[2])
    own_k.start()
    own_v.start()
    own_d.start()

    def q_copy(b):
        return pltpu.make_async_copy(q_in.at[b], q_v.at[b], qg_sem.at[b, 0])

    def g_copy(b):
        return pltpu.make_async_copy(g_in.at[b], g_v.at[b], qg_sem.at[b, 1])

    for b in range(n_batch):
        q_copy(b).start()
        g_copy(b).start()

    barrier = pltpu.get_barrier_semaphore()
    for step in range(1, n_grp):
        pl.semaphore_signal(barrier, inc=1, device_id={'cp': (rank + step) % n_grp},
                            device_id_type=MESH)

    def clear(p, _):
        docs[p] = jnp.zeros(docs.shape[1:], docs.dtype)
        return 0

    lax.fori_loop(rank + 1, n_grp, clear, 0)

    @pl.when(core == 0)
    def _():
        for which in range(2):
            kv[:, which, at(peer), :] = jnp.zeros((n_batch, piece, dim), kv.dtype)

    own_d.wait()
    own = doc_own[...]
    wide = jnp.concatenate([own, own], axis=1)
    lane = lax.broadcasted_iota(jnp.int32, wide.shape, 1)
    docs[rank] = jnp.where(lane // piece == core, wide, 0)
    own_k.wait()
    own_v.wait()
    pl.semaphore_wait(barrier, n_grp - 1)

    def doc_copy(to):
        return remote(docs.at[rank], docs.at[rank], doc_send.at[to], doc_recv.at[rank], to)

    def kv_copy(b, to):
        src = kv.at[b, :, at(rank), :]
        return remote(src, src, kv_send.at[to // CORES], kv_recv.at[b, chip], to)

    def fwd_copy(b, src_chip):
        src = kv.at[b, :, at(src_chip * CORES + core), :]
        return remote(src, src, fwd_send.at[src_chip], fwd_recv.at[b, src_chip], peer)

    for to in range(n_grp):
        @pl.when(to > rank)
        def _():
            doc_copy(to).start()

    def send_own(b):
        @pl.when(core == 0)
        def _():
            kv_copy(b, peer).start()
        for far in range(n_chip - 1, 0, -1):
            @pl.when(far > chip)
            def _():
                kv_copy(b, far * CORES + core).start()

    for b in range(AHEAD):
        send_own(b)

    def kv_arrival(b, src_chip, sem):
        src = kv.at[b, :, at(rank), :]
        return remote(src, src, kv_send.at[0], sem.at[b, src_chip], peer)

    def forward(b):
        for src_chip in range(n_chip - 1):
            @pl.when(src_chip < chip)
            def _():
                kv_arrival(b, src_chip, kv_recv).wait_recv()
                fwd_copy(b, src_chip).start()

    def arrived(b):
        for src_chip in range(n_chip - 1):
            @pl.when(src_chip < chip)
            def _():
                kv_arrival(b, src_chip, fwd_recv).wait_recv()

        @pl.when(core == 1)
        def _():
            kv_arrival(b, chip, kv_recv).wait_recv()

    own_t = wide.T
    for b in range(n_batch):
        qry_doc[b] = jnp.broadcast_to(own_t[:piece, b:b + 1], (piece, LANE))
    forward(0)
    for p in range(n_grp):
        @pl.when(p < rank)
        def _():
            remote(docs.at[p], docs.at[p], doc_send.at[p], doc_recv.at[p], peer).wait_recv()
    for t in range(n_chip):
        ids = docs[CORES * t] + docs[CORES * t + 1]
        for b in range(n_batch):
            key_doc[b, :, t * LANE:(t + 1) * LANE] = ids[b:b + 1]

    def pp_copy(b, t):
        return remote(part.at[b, 1 - core, t], peer_part.at[b, t], pp_send.at[t],
                      pp_recv.at[b, t], peer)

    last = n_chip - 1

    def far_copy(b, t):
        to = t
        if t == 0:
            to = jnp.where(chip == last - 1, last, t)
        if t == 1:
            to = jnp.where((chip == last) & (b % 2 == 0), 0, t)
        slot = chip - t - 1
        return remote(comb.at[b, t], far_part.at[b, slot], far_send.at[t],
                      far_recv.at[b, slot], to * CORES + core)

    def far_arrival(b, slot):
        return remote(comb.at[b, 0], far_part.at[b, slot], far_send.at[0],
                      far_recv.at[b, slot], peer)

    def relay_copy(b):
        return remote(far_part.at[b, 1], far_part.at[b, 1], far_send.at[1],
                      far_recv.at[b, 1], CORES + core)

    def merge(b):
        @pl.when(chip == last)
        def _():
            far_arrival(b, 1).wait_recv()
            comb[b, 0] += far_part[b, 1]

    def send_merged(b):
        @pl.when(chip == last)
        def _():
            far_copy(b, 0).start()

    def tiles(fn):
        for t in range(n_chip):
            @pl.when(t <= chip)
            def _():
                fn(t)

    def combine(b):
        def one(t):
            pp_copy(b, t).wait_recv()
            comb[b, t] = part[b, core, t] + peer_part[b, t]
        tiles(one)

    def send_far(b):
        for t in range(last - 1, -1, -1):
            @pl.when((t < chip) & ((t > 0) | (chip != last)))
            def _():
                far_copy(b, t).start()

    n_blocks = n_rows // ROWS
    toks = ROWS // heads

    def attend(b, keys):
        blocks = [slice(i * ROWS, (i + 1) * ROWS) for i in range(n_blocks)]
        scores = [dot(q_v[b, rows, :], kv[b, 0, 0:keys, :], NT) for rows in blocks]
        probs = []
        for i, rows in enumerate(blocks):
            lim = cap[i * toks:(i + 1) * toks, 0:keys]
            lim = jnp.broadcast_to(lim[:, None, :], (toks, heads, keys)).reshape(ROWS, keys)
            s = jnp.minimum(scores[i], lim)
            top = jnp.max(s, axis=-1, keepdims=True)
            e = jnp.exp2((s - top) * (scale * math.log2(math.e)))
            prob = e * (1.0 / jnp.sum(e, axis=-1, keepdims=True))
            p_low[rows, 0:keys] = prob.astype(jnp.bfloat16)
            probs.append((prob, prob.astype(jnp.bfloat16)))
        grads = []
        for rows, (prob, low) in zip(blocks, probs):
            g = g_v[b, rows, :]
            v = kv[b, 1, 0:keys, :]
            dp = dot(g, v, NT)
            o = dot(low, v).astype(jnp.bfloat16)
            o_v[b, rows, :] = o
            delta = jnp.sum(g.astype(jnp.float32) * o.astype(jnp.float32), axis=-1, keepdims=True)
            ds = (prob * (dp - delta)).astype(jnp.bfloat16)
            d_low[rows, 0:keys] = ds
            grads.append(ds)
        for rows, ds in zip(blocks, grads):
            dq_v[b, rows, :] = (dot(ds, kv[b, 0, 0:keys, :]) * scale).astype(jnp.bfloat16)

    def key_grads(b, keys):
        dv = dot(g_v[b], p_low[:, 0:keys], TN)
        dk = dot(q_v[b], d_low[:, 0:keys], TN)
        for t in range(keys // LANE):
            cols = slice(t * LANE, (t + 1) * LANE)
            part[b, 0, t] = dk[:, cols]
            part[b, 1, t] = dv[:, cols]

    def per_chip(fn, b):
        for c in range(n_chip):
            @pl.when(chip == c)
            def _():
                fn(b, (c + 1) * LANE)

    def out_copies(b):
        return (pltpu.make_async_copy(o_v.at[b], o_out.at[b], out_sem.at[0]),
                pltpu.make_async_copy(dq_v.at[b], dq_out.at[b], out_sem.at[1]))

    def step(b, _):
        @pl.when(b + AHEAD < n_batch)
        def _():
            send_own(b + AHEAD)

        q_copy(b).wait()
        g_copy(b).wait()
        arrived(b)
        q_pos = rank * piece + lax.broadcasted_iota(jnp.int32, (piece, LANE), 0)
        for t in range(n_chip):
            k_pos = t * LANE + lax.broadcasted_iota(jnp.int32, (piece, LANE), 1)
            ids = jnp.broadcast_to(key_doc[b, :, t * LANE:(t + 1) * LANE], (piece, LANE))
            seen = (ids == qry_doc[b]) & (k_pos <= q_pos)
            cap[:, t * LANE:(t + 1) * LANE] = jnp.where(seen, POS_BIG, NEG_BIG)
        per_chip(attend, b)

        @pl.when(b > 0)
        def _():
            combine(b - 1)

        @pl.when(b == 0)
        def _():
            forward(1)

        @pl.when(b + 2 < n_batch)
        def _():
            forward(b + 2)

        @pl.when(b > 0)
        def _():
            send_far(b - 1)

        @pl.when(b > 1)
        def _():
            merge(b - 2)
            send_merged(b - 2)
        per_chip(key_grads, b)
        tiles(lambda t: pp_copy(b, t).start())
        for copy in out_copies(b):
            copy.start()
        return 0

    lax.fori_loop(0, n_batch, step, 0)
    combine(n_batch - 1)
    send_far(n_batch - 1)
    for b in (n_batch - 2, n_batch - 1):
        merge(b)
        send_merged(b)

    def fin_copy(b):
        return remote(fin.at[b, at(1 - core), :], peer_fin.at[b], fin_send.at[0],
                      fin_recv.at[0], peer)

    unit = jnp.where(core == 0, jnp.float32(scale), jnp.float32(1.0))

    def finish(b, _):
        fin_acc = comb[b, chip]
        peer_part[b, 0] = fin_acc
        @pl.when((chip == 0) & (b % 2 == 0))
        def _():
            far_arrival(b, 1).wait_recv()
            relay_copy(b).start()
        for slot in range(last):
            used = slot < last - chip
            if slot == 1:
                used &= chip != 0

            @pl.when(used)
            def _():
                far_arrival(b, slot).wait_recv()
                peer_part[b, 0] += far_part[b, slot]
        fin[b] = (peer_part[b, 0].T * unit).astype(jnp.bfloat16)
        fin_copy(b).start()
        return 0

    lax.fori_loop(0, n_batch, finish, 0)

    fin_all = remote(fin.at[:, at(1 - core), :], peer_fin, fin_send.at[0], fin_recv.at[0], peer)
    fin_all.wait_recv()

    mine = fin.at[:, at(core), :]
    for this in range(CORES):
        @pl.when(core == this)
        def _():
            ours, theirs = (dk_out, dv_out) if this == 0 else (dv_out, dk_out)
            copies = (pltpu.make_async_copy(mine, ours, in_sem.at[0]),
                      pltpu.make_async_copy(peer_fin, theirs, in_sem.at[1]))
            for copy in copies:
                copy.start()
            for copy in copies:
                copy.wait()

    for to in range(n_grp):
        @pl.when(to > rank)
        def _():
            doc_copy(to).wait_send()

    def sent(src, sem):
        remote(src, src, sem, kv_recv.at[0, 0], peer).wait_send()

    own_all = kv.at[:, :, at(rank), :]

    @pl.when(core == 0)
    def _():
        sent(own_all, kv_send.at[chip])
    for far in range(1, n_chip):
        @pl.when(far > chip)
        def _():
            sent(own_all, kv_send.at[far])
    for t in range(last):
        @pl.when(t < chip)
        def _():
            sent(own_all, fwd_send.at[t])
            sent(comb.at[:, t], far_send.at[t])

    @pl.when(chip == 0)
    def _():
        sent(comb.at[0:n_batch // 2, 0], far_send.at[1])
    tiles(lambda t: sent(part.at[:, 0, t], pp_send.at[t]))
    fin_all.wait_send()
    pltpu.make_async_copy(o_v, o_out, out_sem.at[0]).wait()
    pltpu.make_async_copy(dq_v, dq_out, out_sem.at[1]).wait()


def solution(mesh):
    n_grp = mesh.shape['cp']
    n_chip = n_grp // CORES
    seq_spec = P('dp', 'cp', None, None)
    id_spec = P('dp', 'cp')

    def per_device(query, keys, values, grad_out, doc_id):
        n_batch, piece, heads, dim = query.shape
        n_rows = piece * heads
        n_keys = n_grp * piece
        flat = (n_batch, n_rows, dim)
        small = (n_batch, piece, dim)
        bf16, f32, i32 = jnp.bfloat16, jnp.float32, jnp.int32
        any_spec = pl.BlockSpec(memory_space=pl.ANY)
        dma = pltpu.SemaphoreType.DMA
        tile = (dim, LANE)
        outs = pl.pallas_call(
            functools.partial(kernel, n_grp, heads),
            out_shape=[jax.ShapeDtypeStruct(flat, bf16), jax.ShapeDtypeStruct(flat, bf16),
                       jax.ShapeDtypeStruct(small, bf16), jax.ShapeDtypeStruct(small, bf16)],
            in_specs=[any_spec] * 5,
            out_specs=[any_spec] * 4,
            scratch_shapes=[
                pltpu.VMEM(flat, bf16), pltpu.VMEM(flat, bf16),
                pltpu.VMEM(flat, bf16), pltpu.VMEM(flat, bf16),
                pltpu.VMEM((n_batch, 2, n_keys, dim), bf16),
                pltpu.VMEM((n_batch, piece), i32),
                pltpu.VMEM((n_grp, n_batch, LANE), i32),
                pltpu.VMEM((n_batch, 1, n_keys), i32),
                pltpu.VMEM((n_batch, piece, LANE), i32),
                pltpu.VMEM((piece, n_keys), f32),
                pltpu.VMEM((n_rows, n_keys), bf16), pltpu.VMEM((n_rows, n_keys), bf16),
                pltpu.VMEM((n_batch, 2, n_chip) + tile, f32),
                pltpu.VMEM((n_batch, n_chip) + tile, f32),
                pltpu.VMEM((n_batch, n_chip) + tile, f32),
                pltpu.VMEM((n_batch, n_chip - 1) + tile, f32),
                pltpu.VMEM((n_batch, LANE, dim), bf16),
                pltpu.VMEM(small, bf16),
                dma((3,)), dma((n_batch, 2)), dma((n_grp,)), dma((n_grp,)),
                dma((n_chip,)), dma((n_batch, n_chip)),
                dma((n_chip - 1,)), dma((n_batch, n_chip - 1)),
                dma((n_chip,)), dma((n_batch, n_chip)),
                dma((n_chip,)), dma((n_batch, n_chip - 1)),
                dma((1,)), dma((1,)), dma((2,)),
            ],
            compiler_params=pltpu.CompilerParams(
                collective_id=0, has_side_effects=True, vmem_limit_bytes=48 * 2**20),
            name='mqa',
        )(query.reshape(flat), grad_out.reshape(flat), *[pltpu.with_memory_space_constraint(a, pltpu.HBM) for a in
            (keys.reshape(small), values.reshape(small), doc_id)])
        attn_out, grad_query, grad_keys, grad_values = outs
        return (attn_out.reshape(query.shape), grad_query.reshape(query.shape),
                grad_keys.reshape(keys.shape), grad_values.reshape(values.shape))

    return jax.shard_map(per_device, mesh=mesh,
                         in_specs=(seq_spec, seq_spec, seq_spec, seq_spec, id_spec),
                         out_specs=(seq_spec, seq_spec, seq_spec, seq_spec), check_vma=False)
```

```python
import functools
import math

import jax
import jax.numpy as jnp
from jax import lax
from jax.experimental import pallas as pl
from jax.experimental.pallas import tpu as pltpu
from jax.sharding import PartitionSpec as P

NEG_BIG = -1e30
POS_BIG = 3e38
MESH = pl.DeviceIdType.MESH
NT = (((1,), (1,)), ((), ()))
TN = (((0,), (0,)), ((), ()))
CORES = 2
ROWS = 512
AHEAD = 2
LATE = 5
LANE = 128


def dot(a, b, dims=(((1,), (0,)), ((), ()))):
    return lax.dot_general(a, b, dims, preferred_element_type=jnp.float32)


def kernel(n_grp, heads,
           q_in, g_in, k_in, v_in, doc_in,
           o_out, dq_out, dk_out, dv_out,
           q_v, g_v, o_v, dq_v, kv, doc_own, docs, key_doc, qry_doc, cap, p_low, d_low,
           part, peer_part, comb, far_part, fin, peer_fin,
           in_sem, qg_sem, doc_send, doc_recv, kv_send, kv_recv, fwd_send, fwd_recv,
           pp_send, pp_recv, far_send, far_recv, fin_send, fin_recv, out_sem):
    n_batch, n_rows, dim = q_v.shape
    piece = n_rows // heads
    n_keys = n_grp * piece
    n_chip = n_grp // CORES
    scale = dim ** -0.5
    rank = lax.axis_index('cp')
    chip = rank // CORES
    core = rank % CORES
    peer = chip * CORES + (1 - core)

    def at(p):
        return pl.ds(pl.multiple_of(p * piece, piece), piece)

    def remote(src, dst, send, recv, to):
        return pltpu.make_async_remote_copy(
            src_ref=src, dst_ref=dst, send_sem=send, recv_sem=recv,
            device_id={'cp': to}, device_id_type=MESH)

    own_k = pltpu.make_async_copy(k_in, kv.at[:, 0, at(rank), :], in_sem.at[0])
    own_v = pltpu.make_async_copy(v_in, kv.at[:, 1, at(rank), :], in_sem.at[1])
    own_d = pltpu.make_async_copy(doc_in, doc_own, in_sem.at[2])
    own_k.start()
    own_v.start()
    own_d.start()

    def q_copy(b):
        return pltpu.make_async_copy(q_in.at[b], q_v.at[b], qg_sem.at[b, 0])

    def g_copy(b):
        return pltpu.make_async_copy(g_in.at[b], g_v.at[b], qg_sem.at[b, 1])

    for b in range(n_batch):
        q_copy(b).start()
        g_copy(b).start()

    barrier = pltpu.get_barrier_semaphore()
    for step in range(1, n_grp):
        pl.semaphore_signal(barrier, inc=1, device_id={'cp': (rank + step) % n_grp},
                            device_id_type=MESH)

    def clear(p, _):
        docs[p] = jnp.zeros(docs.shape[1:], docs.dtype)
        return 0

    lax.fori_loop(rank + 1, n_grp, clear, 0)

    @pl.when(core == 0)
    def _():
        for which in range(2):
            kv[:, which, at(peer), :] = jnp.zeros((n_batch, piece, dim), kv.dtype)

    own_d.wait()
    own = doc_own[...]
    wide = jnp.concatenate([own, own], axis=1)
    lane = lax.broadcasted_iota(jnp.int32, wide.shape, 1)
    docs[rank] = jnp.where(lane // piece == core, wide, 0)
    own_k.wait()
    own_v.wait()
    pl.semaphore_wait(barrier, n_grp - 1)

    def doc_copy(to):
        return remote(docs.at[rank], docs.at[rank], doc_send.at[to], doc_recv.at[rank], to)

    def kv_copy(b, to):
        src = kv.at[b, :, at(rank), :]
        return remote(src, src, kv_send.at[to // CORES], kv_recv.at[b, chip], to)

    def fwd_copy(b, src_chip):
        src = kv.at[b, :, at(src_chip * CORES + core), :]
        return remote(src, src, fwd_send.at[src_chip], fwd_recv.at[b, src_chip], peer)

    def send_own(b):
        @pl.when(core == 0)
        def _():
            kv_copy(b, peer).start()
        for far in range(n_chip - 1, 0, -1):
            @pl.when(far > chip)
            def _():
                kv_copy(b, far * CORES + core).start()

    send_own(0)
    for to in range(n_grp):
        @pl.when(to > rank)
        def _():
            doc_copy(to).start()

    def kv_arrival(b, src_chip, sem):
        src = kv.at[b, :, at(rank), :]
        return remote(src, src, kv_send.at[0], sem.at[b, src_chip], peer)

    def forward(b, c):
        for src_chip in range(c):
            kv_arrival(b, src_chip, kv_recv).wait_recv()
            fwd_copy(b, src_chip).start()

    def arrived(b):
        for src_chip in range(n_chip - 1):
            @pl.when(src_chip < chip)
            def _():
                kv_arrival(b, src_chip, fwd_recv).wait_recv()

        @pl.when(core == 1)
        def _():
            kv_arrival(b, chip, kv_recv).wait_recv()

    own_t = wide.T
    for b in range(n_batch):
        qry_doc[b] = jnp.broadcast_to(own_t[:piece, b:b + 1], (piece, LANE))
    for b in range(1, AHEAD):
        send_own(b)
    for c in range(1, n_chip):
        @pl.when(chip == c)
        def _():
            forward(0, c)
    for p in range(n_grp):
        @pl.when(p < rank)
        def _():
            remote(docs.at[p], docs.at[p], doc_send.at[p], doc_recv.at[p], peer).wait_recv()
    for t in range(n_chip):
        ids = docs[CORES * t] + docs[CORES * t + 1]
        for b in range(n_batch):
            key_doc[b, :, t * LANE:(t + 1) * LANE] = ids[b:b + 1]

    def pp_copy(b, c):
        return remote(part.at[b, 1 - core, 0:c + 1], peer_part.at[b, 0:c + 1], pp_send.at[0],
                      pp_recv.at[b], peer)

    last = n_chip - 1

    def far_copy(b, t):
        to = t
        if t == 0:
            to = jnp.where(chip == last - 1, last, t)
        if t == 1:
            to = jnp.where((chip == last) & (b % 2 == 0), 0, t)
        slot = chip - t - 1
        return remote(comb.at[b, t], far_part.at[b, slot], far_send.at[t],
                      far_recv.at[b, slot], to * CORES + core)

    def far_arrival(b, slot):
        return remote(comb.at[b, 0], far_part.at[b, slot], far_send.at[0],
                      far_recv.at[b, slot], peer)

    def relay_copy(b):
        return remote(far_part.at[b, 1], far_part.at[b, 1], far_send.at[1],
                      far_recv.at[b, 1], CORES + core)

    def merge(b):
        far_arrival(b, 1).wait_recv()
        comb[b, 0] += far_part[b, 1]
        far_copy(b, 0).start()

    def combine(b, c):
        pp_copy(b, c).wait_recv()
        for t in range(c + 1):
            comb[b, t] = part[b, core, t] + peer_part[b, t]

    def send_far(b, c):
        for t in range(1 if c == last else 0, c):
            far_copy(b, t).start()

    n_blocks = n_rows // ROWS
    toks = ROWS // heads

    def attend(b, keys):
        blocks = [slice(i * ROWS, (i + 1) * ROWS) for i in range(n_blocks)]
        scores = [dot(q_v[b, rows, :], kv[b, 0, 0:keys, :], NT) for rows in blocks]
        probs = []
        for i, rows in enumerate(blocks):
            lim = cap[i * toks:(i + 1) * toks, 0:keys]
            lim = jnp.broadcast_to(lim[:, None, :], (toks, heads, keys)).reshape(ROWS, keys)
            s = jnp.minimum(scores[i], lim)
            top = jnp.max(s, axis=-1, keepdims=True)
            e = jnp.exp2((s - top) * (scale * math.log2(math.e)))
            prob = e * (1.0 / jnp.sum(e, axis=-1, keepdims=True))
            p_low[rows, 0:keys] = prob.astype(jnp.bfloat16)
            probs.append((prob, prob.astype(jnp.bfloat16)))
        grads = []
        for rows, (prob, low) in zip(blocks, probs):
            g = g_v[b, rows, :]
            v = kv[b, 1, 0:keys, :]
            dp = dot(g, v, NT)
            o = dot(low, v).astype(jnp.bfloat16)
            o_v[b, rows, :] = o
            delta = jnp.sum(g.astype(jnp.float32) * o.astype(jnp.float32), axis=-1, keepdims=True)
            ds = (prob * (dp - delta)).astype(jnp.bfloat16)
            d_low[rows, 0:keys] = ds
            grads.append(ds)
        for rows, ds in zip(blocks, grads):
            dq_v[b, rows, :] = (dot(ds, kv[b, 0, 0:keys, :]) * scale).astype(jnp.bfloat16)

    def key_grads(b, keys):
        dv = dot(g_v[b], p_low[:, 0:keys], TN)
        dk = dot(q_v[b], d_low[:, 0:keys], TN)
        for t in range(keys // LANE):
            cols = slice(t * LANE, (t + 1) * LANE)
            part[b, 0, t] = dk[:, cols]
            part[b, 1, t] = dv[:, cols]

    def per_chip(fn):
        for c in range(n_chip):
            @pl.when(chip == c)
            def _():
                fn(c)

    def out_copies(b):
        return (pltpu.make_async_copy(o_v.at[b], o_out.at[b], out_sem.at[0]),
                pltpu.make_async_copy(dq_v.at[b], dq_out.at[b], out_sem.at[1]))

    def step(b, _):
        @pl.when(b + AHEAD < n_batch)
        def _():
            send_own(b + AHEAD)

        q_copy(b).wait()
        g_copy(b).wait()
        arrived(b)
        per_chip(functools.partial(work, b))
        return 0

    def work(b, c):
        q_pos = rank * piece + lax.broadcasted_iota(jnp.int32, (piece, LANE), 0)
        for t in range(c + 1):
            k_pos = t * LANE + lax.broadcasted_iota(jnp.int32, (piece, LANE), 1)
            ids = jnp.broadcast_to(key_doc[b, :, t * LANE:(t + 1) * LANE], (piece, LANE))
            seen = (ids == qry_doc[b]) & (k_pos <= q_pos)
            cap[:, t * LANE:(t + 1) * LANE] = jnp.where(seen, POS_BIG, NEG_BIG)
        attend(b, (c + 1) * LANE)

        @pl.when(b > 0)
        def _():
            combine(b - 1, c)
            send_far(b - 1, c)

        if c > 0:
            @pl.when(b == 0)
            def _():
                forward(1, c)

            @pl.when(b + 2 < n_batch)
            def _():
                forward(b + 2, c)
        if c == last:
            @pl.when((b > 1) & (b <= LATE))
            def _():
                merge(b - 2)

            @pl.when(b >= LATE)
            def _():
                merge(b - 1)
        key_grads(b, (c + 1) * LANE)
        pp_copy(b, c).start()
        for copy in out_copies(b):
            copy.start()

    lax.fori_loop(0, n_batch, step, 0)

    def finish_loop(c):
        combine(n_batch - 1, c)
        send_far(n_batch - 1, c)
        if c == last:
            merge(n_batch - 1)

    per_chip(finish_loop)

    def fin_copy(b):
        return remote(fin.at[b, at(1 - core), :], peer_fin.at[b], fin_send.at[0],
                      fin_recv.at[0], peer)

    unit = jnp.where(core == 0, jnp.float32(scale), jnp.float32(1.0))

    def finish(b, _):
        fin_acc = comb[b, chip]
        peer_part[b, 0] = fin_acc
        @pl.when((chip == 0) & (b % 2 == 0))
        def _():
            far_arrival(b, 1).wait_recv()
            relay_copy(b).start()
        for slot in range(last):
            used = slot < last - chip
            if slot == 1:
                used &= chip != 0

            @pl.when(used)
            def _():
                far_arrival(b, slot).wait_recv()
                peer_part[b, 0] += far_part[b, slot]
        fin[b] = (peer_part[b, 0].T * unit).astype(jnp.bfloat16)
        fin_copy(b).start()
        return 0

    lax.fori_loop(0, n_batch, finish, 0)

    fin_all = remote(fin.at[:, at(1 - core), :], peer_fin, fin_send.at[0], fin_recv.at[0], peer)
    fin_all.wait_recv()

    mine = fin.at[:, at(core), :]
    for this in range(CORES):
        @pl.when(core == this)
        def _():
            ours, theirs = (dk_out, dv_out) if this == 0 else (dv_out, dk_out)
            copies = (pltpu.make_async_copy(mine, ours, in_sem.at[0]),
                      pltpu.make_async_copy(peer_fin, theirs, in_sem.at[1]))
            for copy in copies:
                copy.start()
            for copy in copies:
                copy.wait()

    for to in range(n_grp):
        @pl.when(to > rank)
        def _():
            doc_copy(to).wait_send()

    def sent(src, sem):
        remote(src, src, sem, kv_recv.at[0, 0], peer).wait_send()

    own_all = kv.at[:, :, at(rank), :]

    @pl.when(core == 0)
    def _():
        sent(own_all, kv_send.at[chip])
    for far in range(1, n_chip):
        @pl.when(far > chip)
        def _():
            sent(own_all, kv_send.at[far])
    for t in range(last):
        @pl.when(t < chip)
        def _():
            sent(own_all, fwd_send.at[t])
            sent(comb.at[:, t], far_send.at[t])

    @pl.when(chip == 0)
    def _():
        sent(comb.at[0:n_batch // 2, 0], far_send.at[1])
    per_chip(lambda c: sent(part.at[:, 0, 0:c + 1], pp_send.at[0]))
    fin_all.wait_send()
    pltpu.make_async_copy(o_v, o_out, out_sem.at[0]).wait()
    pltpu.make_async_copy(dq_v, dq_out, out_sem.at[1]).wait()


def write_out(*refs):
    n = (len(refs) - 1) // 2
    copies = [pltpu.make_async_copy(refs[i], refs[n + i], refs[-1].at[i]) for i in range(n)]
    for copy in copies:
        copy.start()
    for copy in copies:
        copy.wait()


def solution(mesh):
    n_grp = mesh.shape['cp']
    n_chip = n_grp // CORES
    seq_spec = P('dp', 'cp', None, None)
    id_spec = P('dp', 'cp')

    def per_device(query, keys, values, grad_out, doc_id):
        n_batch, piece, heads, dim = query.shape
        n_rows = piece * heads
        n_keys = n_grp * piece
        flat = (n_batch, n_rows, dim)
        small = (n_batch, piece, dim)
        bf16, f32, i32 = jnp.bfloat16, jnp.float32, jnp.int32
        any_spec = pl.BlockSpec(memory_space=pl.ANY)
        dma = pltpu.SemaphoreType.DMA
        tile = (dim, LANE)
        outs = pl.pallas_call(
            functools.partial(kernel, n_grp, heads),
            out_shape=[jax.ShapeDtypeStruct(flat, bf16), jax.ShapeDtypeStruct(flat, bf16),
                       jax.ShapeDtypeStruct(small, bf16), jax.ShapeDtypeStruct(small, bf16)],
            in_specs=[any_spec] * 5,
            out_specs=[any_spec] * 4,
            scratch_shapes=[
                pltpu.VMEM(flat, bf16), pltpu.VMEM(flat, bf16),
                pltpu.VMEM(flat, bf16), pltpu.VMEM(flat, bf16),
                pltpu.VMEM((n_batch, 2, n_keys, dim), bf16),
                pltpu.VMEM((n_batch, piece), i32),
                pltpu.VMEM((n_grp, n_batch, LANE), i32),
                pltpu.VMEM((n_batch, 1, n_keys), i32),
                pltpu.VMEM((n_batch, piece, LANE), i32),
                pltpu.VMEM((piece, n_keys), f32),
                pltpu.VMEM((n_rows, n_keys), bf16), pltpu.VMEM((n_rows, n_keys), bf16),
                pltpu.VMEM((n_batch, 2, n_chip) + tile, f32),
                pltpu.VMEM((n_batch, n_chip) + tile, f32),
                pltpu.VMEM((n_batch, n_chip) + tile, f32),
                pltpu.VMEM((n_batch, n_chip - 1) + tile, f32),
                pltpu.VMEM((n_batch, LANE, dim), bf16),
                pltpu.VMEM(small, bf16),
                dma((3,)), dma((n_batch, 2)), dma((n_grp,)), dma((n_grp,)),
                dma((n_chip,)), dma((n_batch, n_chip)),
                dma((n_chip - 1,)), dma((n_batch, n_chip - 1)),
                dma((1,)), dma((n_batch,)),
                dma((n_chip - 1,)), dma((n_batch, n_chip - 1)),
                dma((1,)), dma((1,)), dma((2,)),
            ],
            compiler_params=pltpu.CompilerParams(
                collective_id=0, has_side_effects=True, vmem_limit_bytes=48 * 2**20),
            name='mqa',
        )(query.reshape(flat), grad_out.reshape(flat), *[pltpu.with_memory_space_constraint(a, pltpu.HBM) for a in
            (keys.reshape(small), values.reshape(small), doc_id)])
        attn_out, grad_query, grad_keys, grad_values = pl.pallas_call(
            write_out,
            out_shape=[jax.ShapeDtypeStruct(a.shape, a.dtype) for a in outs],
            in_specs=[any_spec] * 4,
            out_specs=[pl.BlockSpec(memory_space=pltpu.HBM)] * 4,
            scratch_shapes=[dma((4,))],
            compiler_params=pltpu.CompilerParams(vmem_limit_bytes=2**20),
            name='write',
        )(*outs)
        return (attn_out.reshape(query.shape), grad_query.reshape(query.shape),
                grad_keys.reshape(keys.shape), grad_values.reshape(values.shape))

    return jax.shard_map(per_device, mesh=mesh,
                         in_specs=(seq_spec, seq_spec, seq_spec, seq_spec, id_spec),
                         out_specs=(seq_spec, seq_spec, seq_spec, seq_spec), check_vma=False)
```

```python
import functools
import math

import jax
import jax.numpy as jnp
from jax import lax
from jax.experimental import pallas as pl
from jax.experimental.pallas import tpu as pltpu
from jax.sharding import PartitionSpec as P

NEG_BIG = -1e30
POS_BIG = 3e38
MESH = pl.DeviceIdType.MESH
NT = (((1,), (1,)), ((), ()))
TN = (((0,), (0,)), ((), ()))
CORES = 2
ROWS = 512
AHEAD = 2
LATE = 5
LANE = 128


def dot(a, b, dims=(((1,), (0,)), ((), ()))):
    return lax.dot_general(a, b, dims, preferred_element_type=jnp.float32)


def kernel(n_grp, heads,
           q_in, g_in, k_in, v_in, doc_in,
           o_out, dq_out, dk_out, dv_out,
           q_v, g_v, o_v, dq_v, kv, doc_own, docs, key_doc, qry_doc, cap, p_low, d_low,
           part, peer_part, comb, far_part, fin,
           in_sem, qg_sem, doc_send, doc_recv, kv_send, kv_recv, fwd_send, fwd_recv,
           pp_send, pp_recv, far_send, far_recv, out_sem):
    n_batch, n_rows, dim = q_v.shape
    piece = n_rows // heads
    n_keys = n_grp * piece
    n_chip = n_grp // CORES
    scale = dim ** -0.5
    rank = lax.axis_index('cp')
    chip = rank // CORES
    core = rank % CORES
    peer = chip * CORES + (1 - core)

    def at(p):
        return pl.ds(pl.multiple_of(p * piece, piece), piece)

    def remote(src, dst, send, recv, to):
        return pltpu.make_async_remote_copy(
            src_ref=src, dst_ref=dst, send_sem=send, recv_sem=recv,
            device_id={'cp': to}, device_id_type=MESH)

    own_k = pltpu.make_async_copy(k_in, kv.at[:, 0, at(rank), :], in_sem.at[0])
    own_v = pltpu.make_async_copy(v_in, kv.at[:, 1, at(rank), :], in_sem.at[1])
    own_d = pltpu.make_async_copy(doc_in, doc_own, in_sem.at[2])
    own_k.start()
    own_v.start()
    own_d.start()

    def q_copy(b):
        return pltpu.make_async_copy(q_in.at[b], q_v.at[b], qg_sem.at[b, 0])

    def g_copy(b):
        return pltpu.make_async_copy(g_in.at[b], g_v.at[b], qg_sem.at[b, 1])

    for b in range(n_batch):
        q_copy(b).start()
        g_copy(b).start()

    barrier = pltpu.get_barrier_semaphore()
    for step in range(1, n_grp):
        pl.semaphore_signal(barrier, inc=1, device_id={'cp': (rank + step) % n_grp},
                            device_id_type=MESH)

    def clear(p, _):
        docs[p] = jnp.zeros(docs.shape[1:], docs.dtype)
        return 0

    lax.fori_loop(rank + 1, n_grp, clear, 0)

    @pl.when(core == 0)
    def _():
        for which in range(2):
            kv[:, which, at(peer), :] = jnp.zeros((n_batch, piece, dim), kv.dtype)

    own_d.wait()
    own = doc_own[...]
    wide = jnp.concatenate([own, own], axis=1)
    lane = lax.broadcasted_iota(jnp.int32, wide.shape, 1)
    docs[rank] = jnp.where(lane // piece == core, wide, 0)
    own_k.wait()
    own_v.wait()
    pl.semaphore_wait(barrier, n_grp - 1)

    def doc_copy(to):
        return remote(docs.at[rank], docs.at[rank], doc_send.at[to], doc_recv.at[rank], to)

    def kv_copy(b, to):
        src = kv.at[b, :, at(rank), :]
        return remote(src, src, kv_send.at[to // CORES], kv_recv.at[b, chip], to)

    def fwd_copy(b, src_chip):
        src = kv.at[b, :, at(src_chip * CORES + core), :]
        return remote(src, src, fwd_send.at[src_chip], fwd_recv.at[b], peer)

    def send_own(b):
        @pl.when(core == 0)
        def _():
            kv_copy(b, peer).start()
        for far in range(n_chip - 1, 0, -1):
            @pl.when(far > chip)
            def _():
                kv_copy(b, far * CORES + core).start()

    send_own(0)
    for to in range(n_grp):
        @pl.when(to > rank)
        def _():
            doc_copy(to).start()

    def kv_arrival(b, src_chip, sem):
        src = kv.at[b, :, at(rank), :]
        return remote(src, src, kv_send.at[0], sem.at[b, src_chip], peer)

    def forward(b, c):
        for src_chip in range(c):
            kv_arrival(b, src_chip, kv_recv).wait_recv()
            fwd_copy(b, src_chip).start()

    def arrived(b, c):
        if c > 0:
            src = kv.at[b, :, 0:c * piece, :]
            remote(src, src, kv_send.at[0], fwd_recv.at[b], peer).wait_recv()

        @pl.when(core == 1)
        def _():
            kv_arrival(b, c, kv_recv).wait_recv()

    own_t = wide.T
    for b in range(n_batch):
        qry_doc[b] = jnp.broadcast_to(own_t[:piece, b:b + 1], (piece, LANE))
    for b in range(1, AHEAD):
        send_own(b)
    for c in range(1, n_chip):
        @pl.when(chip == c)
        def _():
            forward(0, c)
    for p in range(n_grp):
        @pl.when(p < rank)
        def _():
            remote(docs.at[p], docs.at[p], doc_send.at[p], doc_recv.at[p], peer).wait_recv()
    for t in range(n_chip):
        ids = docs[CORES * t] + docs[CORES * t + 1]
        for b in range(n_batch):
            key_doc[b, :, t * LANE:(t + 1) * LANE] = ids[b:b + 1]

    def pp_copy(b, c):
        return remote(part.at[b, 1 - core, 0:c + 1], peer_part.at[b, 0:c + 1], pp_send.at[0],
                      pp_recv.at[b], peer)

    last = n_chip - 1

    def far_copy(b, t):
        to = t
        if t == 0:
            to = jnp.where(chip == last - 1, last, t)
        if t == 1:
            to = jnp.where((chip == last) & (b % 2 == 0), 0, t)
        slot = chip - t - 1
        return remote(comb.at[b, t], far_part.at[b, slot], far_send.at[t],
                      far_recv.at[b, slot], to * CORES + core)

    def far_arrival(b, slot):
        return remote(comb.at[b, 0], far_part.at[b, slot], far_send.at[0],
                      far_recv.at[b, slot], peer)

    def relay_copy(b):
        return remote(far_part.at[b, 1], far_part.at[b, 1], far_send.at[1],
                      far_recv.at[b, 1], CORES + core)

    def merge(b):
        far_arrival(b, 1).wait_recv()
        comb[b, 0] += far_part[b, 1]
        far_copy(b, 0).start()

    def combine(b, c):
        pp_copy(b, c).wait_recv()
        for t in range(c + 1):
            comb[b, t] = part[b, core, t] + peer_part[b, t]

    def send_far(b, c):
        for t in range(1 if c == last else 0, c):
            far_copy(b, t).start()

    n_blocks = n_rows // ROWS
    toks = ROWS // heads

    def attend(b, keys):
        blocks = [slice(i * ROWS, (i + 1) * ROWS) for i in range(n_blocks)]
        scores = [dot(q_v[b, rows, :], kv[b, 0, 0:keys, :], NT) for rows in blocks]
        probs = []
        for i, rows in enumerate(blocks):
            lim = cap[i * toks:(i + 1) * toks, 0:keys]
            lim = jnp.broadcast_to(lim[:, None, :], (toks, heads, keys)).reshape(ROWS, keys)
            s = jnp.minimum(scores[i], lim)
            top = jnp.max(s, axis=-1, keepdims=True)
            e = jnp.exp2((s - top) * (scale * math.log2(math.e)))
            prob = e * (1.0 / jnp.sum(e, axis=-1, keepdims=True))
            p_low[rows, 0:keys] = prob.astype(jnp.bfloat16)
            probs.append((prob, prob.astype(jnp.bfloat16)))
        grads = []
        for rows, (prob, low) in zip(blocks, probs):
            g = g_v[b, rows, :]
            v = kv[b, 1, 0:keys, :]
            dp = dot(g, v, NT)
            o = dot(low, v).astype(jnp.bfloat16)
            o_v[b, rows, :] = o
            delta = jnp.sum(g.astype(jnp.float32) * o.astype(jnp.float32), axis=-1, keepdims=True)
            ds = (prob * (dp - delta)).astype(jnp.bfloat16)
            d_low[rows, 0:keys] = ds
            grads.append(ds)
        for rows, ds in zip(blocks, grads):
            dq_v[b, rows, :] = (dot(ds, kv[b, 0, 0:keys, :]) * scale).astype(jnp.bfloat16)

    def key_grads(b, keys):
        dv = dot(g_v[b], p_low[:, 0:keys], TN)
        dk = dot(q_v[b], d_low[:, 0:keys], TN)
        left = lax.broadcasted_iota(jnp.int32, (dim, LANE), 1) < piece
        for t in range(keys // LANE):
            cols = slice(t * LANE, (t + 1) * LANE)
            dk_t, dv_t = dk[:, cols], dv[:, cols]
            part[b, 0, t] = jnp.where(left, dk_t, pltpu.roll(dv_t, piece, 1))
            part[b, 1, t] = jnp.where(left, pltpu.roll(dk_t, piece, 1), dv_t)

    def per_chip(fn):
        for c in range(n_chip):
            @pl.when(chip == c)
            def _():
                fn(c)

    def out_copies(b):
        return (pltpu.make_async_copy(o_v.at[b], o_out.at[b], out_sem.at[0]),
                pltpu.make_async_copy(dq_v.at[b], dq_out.at[b], out_sem.at[1]))

    def step(b, _):
        @pl.when(b + AHEAD < n_batch)
        def _():
            send_own(b + AHEAD)

        q_copy(b).wait()
        g_copy(b).wait()
        per_chip(functools.partial(work, b))
        return 0

    def work(b, c):
        arrived(b, c)
        q_pos = rank * piece + lax.broadcasted_iota(jnp.int32, (piece, LANE), 0)
        for t in range(c + 1):
            k_pos = t * LANE + lax.broadcasted_iota(jnp.int32, (piece, LANE), 1)
            ids = jnp.broadcast_to(key_doc[b, :, t * LANE:(t + 1) * LANE], (piece, LANE))
            seen = (ids == qry_doc[b]) & (k_pos <= q_pos)
            cap[:, t * LANE:(t + 1) * LANE] = jnp.where(seen, POS_BIG, NEG_BIG)
        attend(b, (c + 1) * LANE)

        @pl.when(b > 0)
        def _():
            combine(b - 1, c)
            send_far(b - 1, c)

        if c > 0:
            @pl.when(b == 0)
            def _():
                forward(1, c)

            @pl.when(b + 2 < n_batch)
            def _():
                forward(b + 2, c)
        if c == last:
            @pl.when((b > 1) & (b <= LATE))
            def _():
                merge(b - 2)

            @pl.when(b >= LATE)
            def _():
                merge(b - 1)
        key_grads(b, (c + 1) * LANE)
        pp_copy(b, c).start()
        for copy in out_copies(b):
            copy.start()

    lax.fori_loop(0, n_batch, step, 0)

    def finish_loop(c):
        combine(n_batch - 1, c)
        send_far(n_batch - 1, c)
        if c == last:
            merge(n_batch - 1)

    per_chip(finish_loop)

    def finish(b, _):
        fin_acc = comb[b, chip]
        peer_part[b, 0] = fin_acc
        @pl.when((chip == 0) & (b % 2 == 0))
        def _():
            far_arrival(b, 1).wait_recv()
            relay_copy(b).start()
        for slot in range(last):
            used = slot < last - chip
            if slot == 1:
                used &= chip != 0

            @pl.when(used)
            def _():
                far_arrival(b, slot).wait_recv()
                peer_part[b, 0] += far_part[b, slot]
        total = peer_part[b, 0].T
        fin[b, 0] = (total[:piece] * scale).astype(jnp.bfloat16)
        fin[b, 1] = total[piece:].astype(jnp.bfloat16)
        pltpu.make_async_copy(fin.at[b, 0], dk_out.at[b], out_sem.at[2]).start()
        pltpu.make_async_copy(fin.at[b, 1], dv_out.at[b], out_sem.at[3]).start()
        return 0

    lax.fori_loop(0, n_batch, finish, 0)

    for to in range(n_grp):
        @pl.when(to > rank)
        def _():
            doc_copy(to).wait_send()

    def sent(src, sem):
        remote(src, src, sem, kv_recv.at[0, 0], peer).wait_send()

    own_all = kv.at[:, :, at(rank), :]

    @pl.when(core == 0)
    def _():
        sent(own_all, kv_send.at[chip])
    for far in range(1, n_chip):
        @pl.when(far > chip)
        def _():
            sent(own_all, kv_send.at[far])
    for t in range(last):
        @pl.when(t < chip)
        def _():
            sent(own_all, fwd_send.at[t])
            sent(comb.at[:, t], far_send.at[t])

    @pl.when(chip == 0)
    def _():
        sent(comb.at[0:n_batch // 2, 0], far_send.at[1])
    per_chip(lambda c: sent(part.at[:, 0, 0:c + 1], pp_send.at[0]))
    pltpu.make_async_copy(o_v, o_out, out_sem.at[0]).wait()
    pltpu.make_async_copy(dq_v, dq_out, out_sem.at[1]).wait()
    pltpu.make_async_copy(fin.at[:, 0], dk_out, out_sem.at[2]).wait()
    pltpu.make_async_copy(fin.at[:, 1], dv_out, out_sem.at[3]).wait()


def write_out(*refs):
    n = (len(refs) - 1) // 2
    copies = [pltpu.make_async_copy(refs[i], refs[n + i], refs[-1].at[i]) for i in range(n)]
    for copy in copies:
        copy.start()
    for copy in copies:
        copy.wait()


def solution(mesh):
    n_grp = mesh.shape['cp']
    n_chip = n_grp // CORES
    seq_spec = P('dp', 'cp', None, None)
    id_spec = P('dp', 'cp')

    def per_device(query, keys, values, grad_out, doc_id):
        n_batch, piece, heads, dim = query.shape
        n_rows = piece * heads
        n_keys = n_grp * piece
        flat = (n_batch, n_rows, dim)
        small = (n_batch, piece, dim)
        bf16, f32, i32 = jnp.bfloat16, jnp.float32, jnp.int32
        any_spec = pl.BlockSpec(memory_space=pl.ANY)
        dma = pltpu.SemaphoreType.DMA
        tile = (dim, LANE)
        outs = pl.pallas_call(
            functools.partial(kernel, n_grp, heads),
            out_shape=[jax.ShapeDtypeStruct(flat, bf16), jax.ShapeDtypeStruct(flat, bf16),
                       jax.ShapeDtypeStruct(small, bf16), jax.ShapeDtypeStruct(small, bf16)],
            in_specs=[any_spec] * 5,
            out_specs=[any_spec] * 4,
            scratch_shapes=[
                pltpu.VMEM(flat, bf16), pltpu.VMEM(flat, bf16),
                pltpu.VMEM(flat, bf16), pltpu.VMEM(flat, bf16),
                pltpu.VMEM((n_batch, 2, n_keys, dim), bf16),
                pltpu.VMEM((n_batch, piece), i32),
                pltpu.VMEM((n_grp, n_batch, LANE), i32),
                pltpu.VMEM((n_batch, 1, n_keys), i32),
                pltpu.VMEM((n_batch, piece, LANE), i32),
                pltpu.VMEM((piece, n_keys), f32),
                pltpu.VMEM((n_rows, n_keys), bf16), pltpu.VMEM((n_rows, n_keys), bf16),
                pltpu.VMEM((n_batch, 2, n_chip) + tile, f32),
                pltpu.VMEM((n_batch, n_chip) + tile, f32),
                pltpu.VMEM((n_batch, n_chip) + tile, f32),
                pltpu.VMEM((n_batch, n_chip - 1) + tile, f32),
                pltpu.VMEM((n_batch, 2, piece, dim), bf16),
                dma((3,)), dma((n_batch, 2)), dma((n_grp,)), dma((n_grp,)),
                dma((n_chip,)), dma((n_batch, n_chip)),
                dma((n_chip - 1,)), dma((n_batch,)),
                dma((1,)), dma((n_batch,)),
                dma((n_chip - 1,)), dma((n_batch, n_chip - 1)),
                dma((4,)),
            ],
            compiler_params=pltpu.CompilerParams(
                collective_id=0, has_side_effects=True, vmem_limit_bytes=48 * 2**20),
            name='mqa',
        )(query.reshape(flat), grad_out.reshape(flat), *[pltpu.with_memory_space_constraint(a, pltpu.HBM) for a in
            (keys.reshape(small), values.reshape(small), doc_id)])
        attn_out, grad_query, grad_keys, grad_values = pl.pallas_call(
            write_out,
            out_shape=[jax.ShapeDtypeStruct(a.shape, a.dtype) for a in outs],
            in_specs=[any_spec] * 4,
            out_specs=[pl.BlockSpec(memory_space=pltpu.HBM)] * 4,
            scratch_shapes=[dma((4,))],
            compiler_params=pltpu.CompilerParams(vmem_limit_bytes=2**20),
            name='write',
        )(*outs)
        return (attn_out.reshape(query.shape), grad_query.reshape(query.shape),
                grad_keys.reshape(keys.shape), grad_values.reshape(values.shape))

    return jax.shard_map(per_device, mesh=mesh,
                         in_specs=(seq_spec, seq_spec, seq_spec, seq_spec, id_spec),
                         out_specs=(seq_spec, seq_spec, seq_spec, seq_spec), check_vma=False)
```

```python
import functools
import math

import jax
import jax.numpy as jnp
from jax import lax
from jax.experimental import pallas as pl
from jax.experimental.pallas import tpu as pltpu
from jax.sharding import PartitionSpec as P

NEG_BIG = -1e30
POS_BIG = 3e38
MESH = pl.DeviceIdType.MESH
NT = (((1,), (1,)), ((), ()))
TN = (((0,), (0,)), ((), ()))
CORES = 2
ROWS = 512
AHEAD = 3
LATE = 5
LANE = 128


def dot(a, b, dims=(((1,), (0,)), ((), ()))):
    return lax.dot_general(a, b, dims, preferred_element_type=jnp.float32)


def kernel(n_grp, heads,
           q_in, g_in, k_in, v_in, doc_in,
           o_out, dq_out, dk_out, dv_out,
           q_v, g_v, o_v, dq_v, kv, doc_own, docs, key_doc, qry_doc, cap, p_low, d_low,
           part, peer_part, comb, far_part, fin,
           in_sem, qg_sem, doc_send, doc_recv, kv_send, kv_recv, fwd_send, fwd_recv,
           pp_send, pp_recv, far_send, far_recv, out_sem):
    n_batch, n_rows, dim = q_v.shape
    piece = n_rows // heads
    n_keys = n_grp * piece
    n_chip = n_grp // CORES
    scale = dim ** -0.5
    rank = lax.axis_index('cp')
    chip = rank // CORES
    core = rank % CORES
    peer = chip * CORES + (1 - core)

    def at(p):
        return pl.ds(pl.multiple_of(p * piece, piece), piece)

    def remote(src, dst, send, recv, to):
        return pltpu.make_async_remote_copy(
            src_ref=src, dst_ref=dst, send_sem=send, recv_sem=recv,
            device_id={'cp': to}, device_id_type=MESH)

    barrier = pltpu.get_barrier_semaphore()
    for step in range(1, n_grp):
        pl.semaphore_signal(barrier, inc=1, device_id={'cp': (rank + step) % n_grp},
                            device_id_type=MESH)

    own_k = pltpu.make_async_copy(k_in, kv.at[:, 0, at(rank), :], in_sem.at[0])
    own_v = pltpu.make_async_copy(v_in, kv.at[:, 1, at(rank), :], in_sem.at[1])
    own_d = pltpu.make_async_copy(doc_in, doc_own, in_sem.at[2])
    own_k.start()
    own_v.start()
    own_d.start()

    def q_copy(b):
        return pltpu.make_async_copy(q_in.at[b], q_v.at[b], qg_sem.at[b, 0])

    def g_copy(b):
        return pltpu.make_async_copy(g_in.at[b], g_v.at[b], qg_sem.at[b, 1])

    def clear(p, _):
        docs[p] = jnp.zeros(docs.shape[1:], docs.dtype)
        return 0

    lax.fori_loop(rank + 1, n_grp, clear, 0)

    @pl.when(core == 0)
    def _():
        for which in range(2):
            kv[:, which, at(peer), :] = jnp.zeros((n_batch, piece, dim), kv.dtype)

    own_d.wait()
    own = doc_own[...]
    wide = jnp.concatenate([own, own], axis=1)
    lane = lax.broadcasted_iota(jnp.int32, wide.shape, 1)
    docs[rank] = jnp.where(lane // piece == core, wide, 0)
    own_k.wait()
    own_v.wait()
    pl.semaphore_wait(barrier, n_grp - 1)

    def doc_copy(to):
        return remote(docs.at[rank], docs.at[rank], doc_send.at[to], doc_recv.at[rank], to)

    def kv_copy(b, to):
        src = kv.at[b, :, at(rank), :]
        return remote(src, src, kv_send.at[to // CORES], kv_recv.at[b, chip], to)

    def fwd_copy(b, src_chip):
        src = kv.at[b, :, at(src_chip * CORES + core), :]
        return remote(src, src, fwd_send.at[src_chip], fwd_recv.at[b], peer)

    def send_own(b):
        @pl.when(core == 0)
        def _():
            kv_copy(b, peer).start()
        for far in range(n_chip - 1, 0, -1):
            @pl.when(far > chip)
            def _():
                kv_copy(b, far * CORES + core).start()

    send_own(0)
    for to in range(n_grp):
        @pl.when(to > rank)
        def _():
            doc_copy(to).start()

    def kv_arrival(b, src_chip, sem):
        src = kv.at[b, :, at(rank), :]
        return remote(src, src, kv_send.at[0], sem.at[b, src_chip], peer)

    def forward(b, c):
        for src_chip in range(c):
            kv_arrival(b, src_chip, kv_recv).wait_recv()
            fwd_copy(b, src_chip).start()

    def arrived(b, c):
        if c > 0:
            src = kv.at[b, :, 0:c * piece, :]
            remote(src, src, kv_send.at[0], fwd_recv.at[b], peer).wait_recv()

        @pl.when(core == 1)
        def _():
            kv_arrival(b, c, kv_recv).wait_recv()

    own_t = wide.T
    for b in range(n_batch):
        qry_doc[b] = jnp.broadcast_to(own_t[:piece, b:b + 1], (piece, LANE))
    send_own(1)
    for b in range(n_batch):
        q_copy(b).start()
        g_copy(b).start()
    for c in range(1, n_chip):
        @pl.when(chip == c)
        def _():
            forward(0, c)
    for p in range(n_grp):
        @pl.when(p < rank)
        def _():
            remote(docs.at[p], docs.at[p], doc_send.at[p], doc_recv.at[p], peer).wait_recv()
    for t in range(n_chip):
        ids = docs[CORES * t] + docs[CORES * t + 1]
        for b in range(n_batch):
            key_doc[b, :, t * LANE:(t + 1) * LANE] = ids[b:b + 1]

    def pp_copy(b, c):
        return remote(part.at[b, 1 - core, 0:c + 1], peer_part.at[b, 0:c + 1], pp_send.at[0],
                      pp_recv.at[b], peer)

    last = n_chip - 1

    def far_copy(b, t):
        to = t
        if t == 0:
            to = jnp.where(chip == last - 1, last, t)
        if t == 1:
            to = jnp.where((chip == last) & (b % 2 == 0), 0, t)
        slot = chip - t - 1
        return remote(comb.at[b, t], far_part.at[b, slot], far_send.at[t],
                      far_recv.at[b, slot], to * CORES + core)

    def far_arrival(b, slot):
        return remote(comb.at[b, 0], far_part.at[b, slot], far_send.at[0],
                      far_recv.at[b, slot], peer)

    def relay_copy(b):
        return remote(far_part.at[b, 1], far_part.at[b, 1], far_send.at[1],
                      far_recv.at[b, 1], CORES + core)

    def merge(b):
        far_arrival(b, 1).wait_recv()
        comb[b, 0] += far_part[b, 1]
        far_copy(b, 0).start()

    def combine(b, c):
        pp_copy(b, c).wait_recv()
        for t in range(c + 1):
            comb[b, t] = part[b, core, t] + peer_part[b, t]

    def send_far(b, c):
        for t in range(1 if c == last else 0, c):
            far_copy(b, t).start()

    n_blocks = n_rows // ROWS
    toks = ROWS // heads

    def attend(b, keys):
        blocks = [slice(i * ROWS, (i + 1) * ROWS) for i in range(n_blocks)]
        scores = [dot(q_v[b, rows, :], kv[b, 0, 0:keys, :], NT) for rows in blocks]
        probs = []
        for i, rows in enumerate(blocks):
            lim = cap[i * toks:(i + 1) * toks, 0:keys]
            lim = jnp.broadcast_to(lim[:, None, :], (toks, heads, keys)).reshape(ROWS, keys)
            s = jnp.minimum(scores[i], lim)
            top = jnp.max(s, axis=-1, keepdims=True)
            e = jnp.exp2((s - top) * (scale * math.log2(math.e)))
            prob = e * (1.0 / jnp.sum(e, axis=-1, keepdims=True))
            p_low[rows, 0:keys] = prob.astype(jnp.bfloat16)
            probs.append((prob, prob.astype(jnp.bfloat16)))
        grads = []
        for rows, (prob, low) in zip(blocks, probs):
            g = g_v[b, rows, :]
            v = kv[b, 1, 0:keys, :]
            dp = dot(g, v, NT)
            o = dot(low, v).astype(jnp.bfloat16)
            o_v[b, rows, :] = o
            delta = jnp.sum(g.astype(jnp.float32) * o.astype(jnp.float32), axis=-1, keepdims=True)
            ds = (prob * (dp - delta)).astype(jnp.bfloat16)
            d_low[rows, 0:keys] = ds
            grads.append(ds)
        for rows, ds in zip(blocks, grads):
            dq_v[b, rows, :] = (dot(ds, kv[b, 0, 0:keys, :]) * scale).astype(jnp.bfloat16)

    def key_grads(b, keys):
        dv = dot(g_v[b], p_low[:, 0:keys], TN)
        dk = dot(q_v[b], d_low[:, 0:keys], TN)
        left = lax.broadcasted_iota(jnp.int32, (dim, LANE), 1) < piece
        for t in range(keys // LANE):
            cols = slice(t * LANE, (t + 1) * LANE)
            dk_t, dv_t = dk[:, cols], dv[:, cols]
            part[b, 0, t] = jnp.where(left, dk_t, pltpu.roll(dv_t, piece, 1))
            part[b, 1, t] = jnp.where(left, pltpu.roll(dk_t, piece, 1), dv_t)

    def per_chip(fn):
        for c in range(n_chip):
            @pl.when(chip == c)
            def _():
                fn(c)

    def out_copies(b):
        return (pltpu.make_async_copy(o_v.at[b], o_out.at[b], out_sem.at[0]),
                pltpu.make_async_copy(dq_v.at[b], dq_out.at[b], out_sem.at[1]))

    def step(b, _):
        @pl.when(b == 0)
        def _():
            send_own(2)

        q_copy(b).wait()
        g_copy(b).wait()
        per_chip(functools.partial(work, b))
        return 0

    def work(b, c):
        arrived(b, c)
        q_pos = rank * piece + lax.broadcasted_iota(jnp.int32, (piece, LANE), 0)
        for t in range(c + 1):
            k_pos = t * LANE + lax.broadcasted_iota(jnp.int32, (piece, LANE), 1)
            ids = jnp.broadcast_to(key_doc[b, :, t * LANE:(t + 1) * LANE], (piece, LANE))
            seen = (ids == qry_doc[b]) & (k_pos <= q_pos)
            cap[:, t * LANE:(t + 1) * LANE] = jnp.where(seen, POS_BIG, NEG_BIG)
        attend(b, (c + 1) * LANE)

        @pl.when(b + AHEAD < n_batch)
        def _():
            send_own(b + AHEAD)

        @pl.when(b > 0)
        def _():
            combine(b - 1, c)
            send_far(b - 1, c)

        if c > 0:
            @pl.when(b == 0)
            def _():
                forward(1, c)

            @pl.when(b + 2 < n_batch)
            def _():
                forward(b + 2, c)
        if c == last:
            @pl.when((b > 1) & (b <= LATE))
            def _():
                merge(b - 2)

            @pl.when(b >= LATE)
            def _():
                merge(b - 1)
        key_grads(b, (c + 1) * LANE)
        pp_copy(b, c).start()
        for copy in out_copies(b):
            copy.start()

    lax.fori_loop(0, n_batch, step, 0)

    def finish_loop(c):
        combine(n_batch - 1, c)
        send_far(n_batch - 1, c)
        if c == last:
            merge(n_batch - 1)

    per_chip(finish_loop)

    def finish(b, _):
        fin_acc = comb[b, chip]
        peer_part[b, 0] = fin_acc
        @pl.when((chip == 0) & (b % 2 == 0))
        def _():
            far_arrival(b, 1).wait_recv()
            relay_copy(b).start()
        for slot in range(last):
            used = slot < last - chip
            if slot == 1:
                used &= chip != 0

            @pl.when(used)
            def _():
                far_arrival(b, slot).wait_recv()
                peer_part[b, 0] += far_part[b, slot]
        total = peer_part[b, 0].T
        fin[b, 0] = (total[:piece] * scale).astype(jnp.bfloat16)
        fin[b, 1] = total[piece:].astype(jnp.bfloat16)
        pltpu.make_async_copy(fin.at[b, 0], dk_out.at[b], out_sem.at[2]).start()
        pltpu.make_async_copy(fin.at[b, 1], dv_out.at[b], out_sem.at[3]).start()
        return 0

    lax.fori_loop(0, n_batch, finish, 0)

    for to in range(n_grp):
        @pl.when(to > rank)
        def _():
            doc_copy(to).wait_send()

    def sent(src, sem):
        remote(src, src, sem, kv_recv.at[0, 0], peer).wait_send()

    own_all = kv.at[:, :, at(rank), :]

    @pl.when(core == 0)
    def _():
        sent(own_all, kv_send.at[chip])
    for far in range(1, n_chip):
        @pl.when(far > chip)
        def _():
            sent(own_all, kv_send.at[far])
    for t in range(last):
        @pl.when(t < chip)
        def _():
            sent(own_all, fwd_send.at[t])
            sent(comb.at[:, t], far_send.at[t])

    @pl.when(chip == 0)
    def _():
        sent(comb.at[0:n_batch // 2, 0], far_send.at[1])
    per_chip(lambda c: sent(part.at[:, 0, 0:c + 1], pp_send.at[0]))
    pltpu.make_async_copy(o_v, o_out, out_sem.at[0]).wait()
    pltpu.make_async_copy(dq_v, dq_out, out_sem.at[1]).wait()
    pltpu.make_async_copy(fin.at[:, 0], dk_out, out_sem.at[2]).wait()
    pltpu.make_async_copy(fin.at[:, 1], dv_out, out_sem.at[3]).wait()


def write_out(*refs):
    n = (len(refs) - 1) // 2
    copies = [pltpu.make_async_copy(refs[i], refs[n + i], refs[-1].at[i]) for i in range(n)]
    for copy in copies:
        copy.start()
    for copy in copies:
        copy.wait()


def solution(mesh):
    n_grp = mesh.shape['cp']
    n_chip = n_grp // CORES
    seq_spec = P('dp', 'cp', None, None)
    id_spec = P('dp', 'cp')

    def per_device(query, keys, values, grad_out, doc_id):
        n_batch, piece, heads, dim = query.shape
        n_rows = piece * heads
        n_keys = n_grp * piece
        flat = (n_batch, n_rows, dim)
        small = (n_batch, piece, dim)
        bf16, f32, i32 = jnp.bfloat16, jnp.float32, jnp.int32
        any_spec = pl.BlockSpec(memory_space=pl.ANY)
        dma = pltpu.SemaphoreType.DMA
        tile = (dim, LANE)
        outs = pl.pallas_call(
            functools.partial(kernel, n_grp, heads),
            out_shape=[jax.ShapeDtypeStruct(flat, bf16), jax.ShapeDtypeStruct(flat, bf16),
                       jax.ShapeDtypeStruct(small, bf16), jax.ShapeDtypeStruct(small, bf16)],
            in_specs=[any_spec] * 5,
            out_specs=[any_spec] * 4,
            scratch_shapes=[
                pltpu.VMEM(flat, bf16), pltpu.VMEM(flat, bf16),
                pltpu.VMEM(flat, bf16), pltpu.VMEM(flat, bf16),
                pltpu.VMEM((n_batch, 2, n_keys, dim), bf16),
                pltpu.VMEM((n_batch, piece), i32),
                pltpu.VMEM((n_grp, n_batch, LANE), i32),
                pltpu.VMEM((n_batch, 1, n_keys), i32),
                pltpu.VMEM((n_batch, piece, LANE), i32),
                pltpu.VMEM((piece, n_keys), f32),
                pltpu.VMEM((n_rows, n_keys), bf16), pltpu.VMEM((n_rows, n_keys), bf16),
                pltpu.VMEM((n_batch, 2, n_chip) + tile, f32),
                pltpu.VMEM((n_batch, n_chip) + tile, f32),
                pltpu.VMEM((n_batch, n_chip) + tile, f32),
                pltpu.VMEM((n_batch, n_chip - 1) + tile, f32),
                pltpu.VMEM((n_batch, 2, piece, dim), bf16),
                dma((3,)), dma((n_batch, 2)), dma((n_grp,)), dma((n_grp,)),
                dma((n_chip,)), dma((n_batch, n_chip)),
                dma((n_chip - 1,)), dma((n_batch,)),
                dma((1,)), dma((n_batch,)),
                dma((n_chip - 1,)), dma((n_batch, n_chip - 1)),
                dma((4,)),
            ],
            compiler_params=pltpu.CompilerParams(
                collective_id=0, has_side_effects=True, vmem_limit_bytes=48 * 2**20),
            name='mqa',
        )(query.reshape(flat), grad_out.reshape(flat), *[pltpu.with_memory_space_constraint(a, pltpu.HBM) for a in
            (keys.reshape(small), values.reshape(small), doc_id)])
        attn_out, grad_query, grad_keys, grad_values = pl.pallas_call(
            write_out,
            out_shape=[jax.ShapeDtypeStruct(a.shape, a.dtype) for a in outs],
            in_specs=[any_spec] * 4,
            out_specs=[pl.BlockSpec(memory_space=pltpu.HBM)] * 4,
            scratch_shapes=[dma((4,))],
            compiler_params=pltpu.CompilerParams(vmem_limit_bytes=2**20),
            name='write',
        )(*outs)
        return (attn_out.reshape(query.shape), grad_query.reshape(query.shape),
                grad_keys.reshape(keys.shape), grad_values.reshape(values.shape))

    return jax.shard_map(per_device, mesh=mesh,
                         in_specs=(seq_spec, seq_spec, seq_spec, seq_spec, id_spec),
                         out_specs=(seq_spec, seq_spec, seq_spec, seq_spec), check_vma=False)
```

```python
import functools
import math

import jax
import jax.numpy as jnp
from jax import lax
from jax.experimental import pallas as pl
from jax.experimental.pallas import tpu as pltpu
from jax.sharding import PartitionSpec as P

NEG_BIG = -1e30
POS_BIG = 3e38
MESH = pl.DeviceIdType.MESH
NT = (((1,), (1,)), ((), ()))
TN = (((0,), (0,)), ((), ()))
CORES = 2
ROWS = 512
AHEAD = 3
LATE = 5
LANE = 128


def dot(a, b, dims=(((1,), (0,)), ((), ()))):
    return lax.dot_general(a, b, dims, preferred_element_type=jnp.float32)


def kernel(n_grp, heads,
           q_in, g_in, k_in, v_in, doc_in,
           o_out, dq_out, dk_out, dv_out,
           q_v, g_v, o_v, dq_v, kv, doc_own, docs, key_doc, qry_doc, cap, p_low, d_low,
           part, peer_part, comb, far_part, fin,
           in_sem, qg_sem, doc_send, doc_recv, kv_send, kv_recv, fwd_send, fwd_recv,
           pp_send, pp_recv, far_send, far_recv, out_sem):
    n_batch, n_rows, dim = q_v.shape
    piece = n_rows // heads
    n_keys = n_grp * piece
    n_chip = n_grp // CORES
    scale = dim ** -0.5
    rank = lax.axis_index('cp')
    chip = rank // CORES
    core = rank % CORES
    peer = chip * CORES + (1 - core)

    def at(p):
        return pl.ds(pl.multiple_of(p * piece, piece), piece)

    def remote(src, dst, send, recv, to):
        return pltpu.make_async_remote_copy(
            src_ref=src, dst_ref=dst, send_sem=send, recv_sem=recv,
            device_id={'cp': to}, device_id_type=MESH)

    barrier = pltpu.get_barrier_semaphore()
    for step in range(1, n_grp):
        pl.semaphore_signal(barrier, inc=1, device_id={'cp': (rank + step) % n_grp},
                            device_id_type=MESH)

    own_k = pltpu.make_async_copy(k_in, kv.at[:, 0, at(rank), :], in_sem.at[0])
    own_v = pltpu.make_async_copy(v_in, kv.at[:, 1, at(rank), :], in_sem.at[1])
    own_d = pltpu.make_async_copy(doc_in, doc_own, in_sem.at[2])
    own_k.start()
    own_v.start()
    own_d.start()

    def q_copy(b):
        return pltpu.make_async_copy(q_in.at[b], q_v.at[b], qg_sem.at[b, 0])

    def g_copy(b):
        return pltpu.make_async_copy(g_in.at[b], g_v.at[b], qg_sem.at[b, 1])

    def clear(p, _):
        docs[p] = jnp.zeros(docs.shape[1:], docs.dtype)
        return 0

    lax.fori_loop(rank + 1, n_grp, clear, 0)

    @pl.when(core == 0)
    def _():
        for which in range(2):
            kv[:, which, at(peer), :] = jnp.zeros((n_batch, piece, dim), kv.dtype)

    own_d.wait()
    own = doc_own[...]
    wide = jnp.concatenate([own, own], axis=1)
    lane = lax.broadcasted_iota(jnp.int32, wide.shape, 1)
    docs[rank] = jnp.where(lane // piece == core, wide, 0)
    own_k.wait()
    own_v.wait()
    pl.semaphore_wait(barrier, n_grp - 1)

    def doc_copy(to):
        return remote(docs.at[rank], docs.at[rank], doc_send.at[to], doc_recv.at[rank], to)

    def kv_copy(b, to):
        src = kv.at[b, :, at(rank), :]
        return remote(src, src, kv_send.at[to // CORES], kv_recv.at[b, chip], to)

    def fwd_copy(b, src_chip):
        src = kv.at[b, :, at(src_chip * CORES + core), :]
        return remote(src, src, fwd_send.at[src_chip], fwd_recv.at[b], peer)

    def send_own(b):
        @pl.when(core == 0)
        def _():
            kv_copy(b, peer).start()
        for far in range(n_chip - 1, 0, -1):
            @pl.when(far > chip)
            def _():
                kv_copy(b, far * CORES + core).start()

    send_own(0)
    for to in range(n_grp):
        @pl.when(to > rank)
        def _():
            doc_copy(to).start()

    def kv_arrival(b, src_chip, sem):
        src = kv.at[b, :, at(rank), :]
        return remote(src, src, kv_send.at[0], sem.at[b, src_chip], peer)

    def forward(b, c):
        for src_chip in range(c):
            kv_arrival(b, src_chip, kv_recv).wait_recv()
            fwd_copy(b, src_chip).start()

    def arrived(b, c):
        if c > 0:
            src = kv.at[b, :, 0:c * piece, :]
            remote(src, src, kv_send.at[0], fwd_recv.at[b], peer).wait_recv()

        @pl.when(core == 1)
        def _():
            kv_arrival(b, c, kv_recv).wait_recv()

    own_t = wide.T
    for b in range(n_batch):
        qry_doc[b] = jnp.broadcast_to(own_t[:piece, b:b + 1], (piece, LANE))
    send_own(1)
    for b in range(n_batch):
        q_copy(b).start()
        g_copy(b).start()
    for c in range(1, n_chip):
        @pl.when(chip == c)
        def _():
            forward(0, c)
    for p in range(n_grp):
        @pl.when(p < rank)
        def _():
            remote(docs.at[p], docs.at[p], doc_send.at[p], doc_recv.at[p], peer).wait_recv()
    for t in range(n_chip):
        ids = docs[CORES * t] + docs[CORES * t + 1]
        for b in range(n_batch):
            key_doc[b, :, t * LANE:(t + 1) * LANE] = ids[b:b + 1]

    def pp_copy(b, c):
        return remote(part.at[b, 1 - core, 0:c + 1], peer_part.at[b, 0:c + 1], pp_send.at[0],
                      pp_recv.at[b], peer)

    last = n_chip - 1

    def over(b):
        return (b % 2 == 0) & (b < n_batch - 2)

    def far_copy(b, t):
        to = t
        if t == 0:
            to = jnp.where(chip == last - 1, last, t)
        if t == 1:
            to = jnp.where((chip == last) & over(b), 0, t)
        slot = chip - t - 1
        return remote(comb.at[b, t], far_part.at[b, slot], far_send.at[t],
                      far_recv.at[b, slot], to * CORES + core)

    def far_arrival(b, slot):
        return remote(comb.at[b, 0], far_part.at[b, slot], far_send.at[0],
                      far_recv.at[b, slot], peer)

    def relay_copy(b):
        return remote(far_part.at[b, 1], far_part.at[b, 1], far_send.at[1],
                      far_recv.at[b, 1], CORES + core)

    def merge(b):
        far_arrival(b, 1).wait_recv()
        comb[b, 0] += far_part[b, 1]
        far_copy(b, 0).start()

    def combine(b, c):
        pp_copy(b, c).wait_recv()
        for t in range(c + 1):
            comb[b, t] = part[b, core, t] + peer_part[b, t]

    def send_far(b, c):
        for t in range(1 if c == last else 0, c):
            far_copy(b, t).start()

    n_blocks = n_rows // ROWS
    toks = ROWS // heads

    def attend(b, keys):
        blocks = [slice(i * ROWS, (i + 1) * ROWS) for i in range(n_blocks)]
        scores = [dot(q_v[b, rows, :], kv[b, 0, 0:keys, :], NT) for rows in blocks]
        probs = []
        for i, rows in enumerate(blocks):
            lim = cap[i * toks:(i + 1) * toks, 0:keys]
            lim = jnp.broadcast_to(lim[:, None, :], (toks, heads, keys)).reshape(ROWS, keys)
            s = jnp.minimum(scores[i], lim)
            top = jnp.max(s, axis=-1, keepdims=True)
            e = jnp.exp2((s - top) * (scale * math.log2(math.e)))
            prob = e * (1.0 / jnp.sum(e, axis=-1, keepdims=True))
            p_low[rows, 0:keys] = prob.astype(jnp.bfloat16)
            probs.append((prob, prob.astype(jnp.bfloat16)))
        grads = []
        for rows, (prob, low) in zip(blocks, probs):
            g = g_v[b, rows, :]
            v = kv[b, 1, 0:keys, :]
            dp = dot(g, v, NT)
            o = dot(low, v).astype(jnp.bfloat16)
            o_v[b, rows, :] = o
            delta = jnp.sum(g.astype(jnp.float32) * o.astype(jnp.float32), axis=-1, keepdims=True)
            ds = (prob * (dp - delta)).astype(jnp.bfloat16)
            d_low[rows, 0:keys] = ds
            grads.append(ds)
        for rows, ds in zip(blocks, grads):
            dq_v[b, rows, :] = (dot(ds, kv[b, 0, 0:keys, :]) * scale).astype(jnp.bfloat16)

    def key_grads(b, keys):
        dv = dot(g_v[b], p_low[:, 0:keys], TN)
        dk = dot(q_v[b], d_low[:, 0:keys], TN)
        left = lax.broadcasted_iota(jnp.int32, (dim, LANE), 1) < piece
        for t in range(keys // LANE):
            cols = slice(t * LANE, (t + 1) * LANE)
            dk_t, dv_t = dk[:, cols], dv[:, cols]
            part[b, 0, t] = jnp.where(left, dk_t, pltpu.roll(dv_t, piece, 1))
            part[b, 1, t] = jnp.where(left, pltpu.roll(dk_t, piece, 1), dv_t)

    def per_chip(fn):
        for c in range(n_chip):
            @pl.when(chip == c)
            def _():
                fn(c)

    def out_copies(b):
        return (pltpu.make_async_copy(o_v.at[b], o_out.at[b], out_sem.at[0]),
                pltpu.make_async_copy(dq_v.at[b], dq_out.at[b], out_sem.at[1]))

    def step(b, _):
        @pl.when(b == 0)
        def _():
            send_own(2)

        q_copy(b).wait()
        g_copy(b).wait()
        per_chip(functools.partial(work, b))
        return 0

    def work(b, c):
        arrived(b, c)
        q_pos = rank * piece + lax.broadcasted_iota(jnp.int32, (piece, LANE), 0)
        for t in range(c + 1):
            k_pos = t * LANE + lax.broadcasted_iota(jnp.int32, (piece, LANE), 1)
            ids = jnp.broadcast_to(key_doc[b, :, t * LANE:(t + 1) * LANE], (piece, LANE))
            seen = (ids == qry_doc[b]) & (k_pos <= q_pos)
            cap[:, t * LANE:(t + 1) * LANE] = jnp.where(seen, POS_BIG, NEG_BIG)
        attend(b, (c + 1) * LANE)

        @pl.when(b + AHEAD < n_batch)
        def _():
            send_own(b + AHEAD)

        @pl.when(b > 0)
        def _():
            combine(b - 1, c)
            send_far(b - 1, c)

        if c > 0:
            @pl.when(b == 0)
            def _():
                forward(1, c)

            @pl.when(b + 2 < n_batch)
            def _():
                forward(b + 2, c)
        if c == last:
            @pl.when((b > 1) & (b <= LATE))
            def _():
                merge(b - 2)

            @pl.when(b >= LATE)
            def _():
                merge(b - 1)
        key_grads(b, (c + 1) * LANE)
        pp_copy(b, c).start()
        for copy in out_copies(b):
            copy.start()

    lax.fori_loop(0, n_batch, step, 0)

    def finish_loop(c):
        combine(n_batch - 1, c)
        send_far(n_batch - 1, c)
        if c == last:
            merge(n_batch - 1)

    per_chip(finish_loop)

    def finish(b, _):
        fin_acc = comb[b, chip]
        peer_part[b, 0] = fin_acc
        @pl.when((chip == 0) & over(b))
        def _():
            far_arrival(b, 1).wait_recv()
            relay_copy(b).start()
        for slot in range(last):
            used = slot < last - chip
            if slot == 1:
                used &= chip != 0

            @pl.when(used)
            def _():
                far_arrival(b, slot).wait_recv()
                peer_part[b, 0] += far_part[b, slot]
        total = peer_part[b, 0].T
        fin[b, 0] = (total[:piece] * scale).astype(jnp.bfloat16)
        fin[b, 1] = total[piece:].astype(jnp.bfloat16)
        pltpu.make_async_copy(fin.at[b, 0], dk_out.at[b], out_sem.at[2]).start()
        pltpu.make_async_copy(fin.at[b, 1], dv_out.at[b], out_sem.at[3]).start()
        return 0

    lax.fori_loop(0, n_batch, finish, 0)

    for to in range(n_grp):
        @pl.when(to > rank)
        def _():
            doc_copy(to).wait_send()

    def sent(src, sem):
        remote(src, src, sem, kv_recv.at[0, 0], peer).wait_send()

    own_all = kv.at[:, :, at(rank), :]

    @pl.when(core == 0)
    def _():
        sent(own_all, kv_send.at[chip])
    for far in range(1, n_chip):
        @pl.when(far > chip)
        def _():
            sent(own_all, kv_send.at[far])
    for t in range(last):
        @pl.when(t < chip)
        def _():
            sent(own_all, fwd_send.at[t])
            sent(comb.at[:, t], far_send.at[t])

    @pl.when(chip == 0)
    def _():
        sent(comb.at[0:n_batch // 2 - 1, 0], far_send.at[1])
    per_chip(lambda c: sent(part.at[:, 0, 0:c + 1], pp_send.at[0]))
    pltpu.make_async_copy(o_v, o_out, out_sem.at[0]).wait()
    pltpu.make_async_copy(dq_v, dq_out, out_sem.at[1]).wait()
    pltpu.make_async_copy(fin.at[:, 0], dk_out, out_sem.at[2]).wait()
    pltpu.make_async_copy(fin.at[:, 1], dv_out, out_sem.at[3]).wait()


def write_out(*refs):
    n = (len(refs) - 1) // 2
    copies = [pltpu.make_async_copy(refs[i], refs[n + i], refs[-1].at[i]) for i in range(n)]
    for copy in copies:
        copy.start()
    for copy in copies:
        copy.wait()


def solution(mesh):
    n_grp = mesh.shape['cp']
    n_chip = n_grp // CORES
    seq_spec = P('dp', 'cp', None, None)
    id_spec = P('dp', 'cp')

    def per_device(query, keys, values, grad_out, doc_id):
        n_batch, piece, heads, dim = query.shape
        n_rows = piece * heads
        n_keys = n_grp * piece
        flat = (n_batch, n_rows, dim)
        small = (n_batch, piece, dim)
        bf16, f32, i32 = jnp.bfloat16, jnp.float32, jnp.int32
        any_spec = pl.BlockSpec(memory_space=pl.ANY)
        dma = pltpu.SemaphoreType.DMA
        tile = (dim, LANE)
        outs = pl.pallas_call(
            functools.partial(kernel, n_grp, heads),
            out_shape=[jax.ShapeDtypeStruct(flat, bf16), jax.ShapeDtypeStruct(flat, bf16),
                       jax.ShapeDtypeStruct(small, bf16), jax.ShapeDtypeStruct(small, bf16)],
            in_specs=[any_spec] * 5,
            out_specs=[any_spec] * 4,
            scratch_shapes=[
                pltpu.VMEM(flat, bf16), pltpu.VMEM(flat, bf16),
                pltpu.VMEM(flat, bf16), pltpu.VMEM(flat, bf16),
                pltpu.VMEM((n_batch, 2, n_keys, dim), bf16),
                pltpu.VMEM((n_batch, piece), i32),
                pltpu.VMEM((n_grp, n_batch, LANE), i32),
                pltpu.VMEM((n_batch, 1, n_keys), i32),
                pltpu.VMEM((n_batch, piece, LANE), i32),
                pltpu.VMEM((piece, n_keys), f32),
                pltpu.VMEM((n_rows, n_keys), bf16), pltpu.VMEM((n_rows, n_keys), bf16),
                pltpu.VMEM((n_batch, 2, n_chip) + tile, f32),
                pltpu.VMEM((n_batch, n_chip) + tile, f32),
                pltpu.VMEM((n_batch, n_chip) + tile, f32),
                pltpu.VMEM((n_batch, n_chip - 1) + tile, f32),
                pltpu.VMEM((n_batch, 2, piece, dim), bf16),
                dma((3,)), dma((n_batch, 2)), dma((n_grp,)), dma((n_grp,)),
                dma((n_chip,)), dma((n_batch, n_chip)),
                dma((n_chip - 1,)), dma((n_batch,)),
                dma((1,)), dma((n_batch,)),
                dma((n_chip - 1,)), dma((n_batch, n_chip - 1)),
                dma((4,)),
            ],
            compiler_params=pltpu.CompilerParams(
                collective_id=0, has_side_effects=True, vmem_limit_bytes=48 * 2**20),
            name='mqa',
        )(query.reshape(flat), grad_out.reshape(flat), *[pltpu.with_memory_space_constraint(a, pltpu.HBM) for a in
            (keys.reshape(small), values.reshape(small), doc_id)])
        attn_out, grad_query, grad_keys, grad_values = pl.pallas_call(
            write_out,
            out_shape=[jax.ShapeDtypeStruct(a.shape, a.dtype) for a in outs],
            in_specs=[any_spec] * 4,
            out_specs=[pl.BlockSpec(memory_space=pltpu.HBM)] * 4,
            scratch_shapes=[dma((4,))],
            compiler_params=pltpu.CompilerParams(vmem_limit_bytes=2**20),
            name='write',
        )(*outs)
        return (attn_out.reshape(query.shape), grad_query.reshape(query.shape),
                grad_keys.reshape(keys.shape), grad_values.reshape(values.shape))

    return jax.shard_map(per_device, mesh=mesh,
                         in_specs=(seq_spec, seq_spec, seq_spec, seq_spec, id_spec),
                         out_specs=(seq_spec, seq_spec, seq_spec, seq_spec), check_vma=False)
```

```python
import functools
import math

import jax
import jax.numpy as jnp
from jax import lax
from jax.experimental import pallas as pl
from jax.experimental.pallas import tpu as pltpu
from jax.sharding import PartitionSpec as P

NEG_BIG = -1e30
POS_BIG = 3e38
MESH = pl.DeviceIdType.MESH
NT = (((1,), (1,)), ((), ()))
TN = (((0,), (0,)), ((), ()))
CORES = 2
ROWS = 512
AHEAD = 3
LATE = 5
LANE = 128


def dot(a, b, dims=(((1,), (0,)), ((), ()))):
    return lax.dot_general(a, b, dims, preferred_element_type=jnp.float32)


def kernel(n_grp, heads,
           q_in, g_in, k_in, v_in, doc_in,
           o_out, dq_out, dk_out, dv_out,
           q_v, g_v, o_v, dq_v, kv, doc_own, docs, key_doc, qry_doc, cap, p_low, d_low,
           part, peer_part, comb, far_part, fin,
           in_sem, qg_sem, doc_send, doc_recv, kv_send, kv_recv, fwd_send, fwd_recv,
           pp_send, pp_recv, far_send, far_recv, out_sem):
    n_batch, n_rows, dim = q_v.shape
    piece = n_rows // heads
    n_keys = n_grp * piece
    n_chip = n_grp // CORES
    scale = dim ** -0.5
    rank = lax.axis_index('cp')
    chip = rank // CORES
    core = rank % CORES
    peer = chip * CORES + (1 - core)

    def at(p):
        return pl.ds(pl.multiple_of(p * piece, piece), piece)

    def remote(src, dst, send, recv, to):
        return pltpu.make_async_remote_copy(
            src_ref=src, dst_ref=dst, send_sem=send, recv_sem=recv,
            device_id={'cp': to}, device_id_type=MESH)

    barrier = pltpu.get_barrier_semaphore()
    for step in range(1, n_grp):
        pl.semaphore_signal(barrier, inc=1, device_id={'cp': (rank + step) % n_grp},
                            device_id_type=MESH)

    own_k = pltpu.make_async_copy(k_in, kv.at[:, 0, at(rank), :], in_sem.at[0])
    own_v = pltpu.make_async_copy(v_in, kv.at[:, 1, at(rank), :], in_sem.at[1])
    own_d = pltpu.make_async_copy(doc_in, doc_own, in_sem.at[2])
    own_k.start()
    own_v.start()
    own_d.start()

    def q_copy(b):
        return pltpu.make_async_copy(q_in.at[b], q_v.at[b], qg_sem.at[b, 0])

    def g_copy(b):
        return pltpu.make_async_copy(g_in.at[b], g_v.at[b], qg_sem.at[b, 1])

    def clear(p, _):
        docs[p] = jnp.zeros(docs.shape[1:], docs.dtype)
        return 0

    lax.fori_loop(rank + 1, n_grp, clear, 0)

    @pl.when(core == 0)
    def _():
        for which in range(2):
            kv[:, which, at(peer), :] = jnp.zeros((n_batch, piece, dim), kv.dtype)

    own_d.wait()
    own = doc_own[...]
    wide = jnp.concatenate([own, own], axis=1)
    lane = lax.broadcasted_iota(jnp.int32, wide.shape, 1)
    docs[rank] = jnp.where(lane // piece == core, wide, 0)
    own_k.wait()
    own_v.wait()
    pl.semaphore_wait(barrier, n_grp - 1)

    def doc_copy(to):
        return remote(docs.at[rank], docs.at[rank], doc_send.at[to], doc_recv.at[rank], to)

    def kv_copy(b, to):
        src = kv.at[b, :, at(rank), :]
        return remote(src, src, kv_send.at[to // CORES], kv_recv.at[b, chip], to)

    def fwd_copy(b, src_chip):
        src = kv.at[b, :, at(src_chip * CORES + core), :]
        return remote(src, src, fwd_send.at[src_chip], fwd_recv.at[b], peer)

    def send_own(b):
        @pl.when(core == 0)
        def _():
            kv_copy(b, peer).start()
        for far in range(n_chip - 1, 0, -1):
            @pl.when(far > chip)
            def _():
                kv_copy(b, far * CORES + core).start()

    send_own(0)
    for to in range(n_grp):
        @pl.when(to > rank)
        def _():
            doc_copy(to).start()

    def kv_arrival(b, src_chip, sem):
        src = kv.at[b, :, at(rank), :]
        return remote(src, src, kv_send.at[0], sem.at[b, src_chip], peer)

    def forward(b, c):
        for src_chip in range(c):
            kv_arrival(b, src_chip, kv_recv).wait_recv()
            fwd_copy(b, src_chip).start()

    def arrived(b, c):
        if c > 0:
            src = kv.at[b, :, 0:c * piece, :]
            remote(src, src, kv_send.at[0], fwd_recv.at[b], peer).wait_recv()

        @pl.when(core == 1)
        def _():
            kv_arrival(b, c, kv_recv).wait_recv()

    own_t = wide.T
    for b in range(n_batch):
        qry_doc[b] = jnp.broadcast_to(own_t[:piece, b:b + 1], (piece, LANE))
    send_own(1)
    for b in range(n_batch):
        q_copy(b).start()
        g_copy(b).start()
    for c in range(1, n_chip):
        @pl.when(chip == c)
        def _():
            forward(0, c)
    for p in range(n_grp):
        @pl.when(p < rank)
        def _():
            remote(docs.at[p], docs.at[p], doc_send.at[p], doc_recv.at[p], peer).wait_recv()
    for t in range(n_chip):
        ids = docs[CORES * t] + docs[CORES * t + 1]
        for b in range(n_batch):
            key_doc[b, :, t * LANE:(t + 1) * LANE] = ids[b:b + 1]

    def pp_copy(b, c):
        return remote(part.at[b, 1 - core, 0:c + 1], peer_part.at[b, 0:c + 1], pp_send.at[0],
                      pp_recv.at[b], peer)

    last = n_chip - 1

    def over(b):
        return (b == 1) | (b == 3) | (b == 4)

    def far_copy(b, t):
        to = t
        if t == 0:
            to = jnp.where(chip == last - 1, last, t)
        if t == 1:
            to = jnp.where((chip == last) & over(b), 0, t)
        slot = chip - t - 1
        return remote(comb.at[b, t], far_part.at[b, slot], far_send.at[t],
                      far_recv.at[b, slot], to * CORES + core)

    def far_arrival(b, slot):
        return remote(comb.at[b, 0], far_part.at[b, slot], far_send.at[0],
                      far_recv.at[b, slot], peer)

    def relay_copy(b):
        return remote(far_part.at[b, 1], far_part.at[b, 1], far_send.at[1],
                      far_recv.at[b, 1], CORES + core)

    def merge(b):
        far_arrival(b, 1).wait_recv()
        comb[b, 0] += far_part[b, 1]
        far_copy(b, 0).start()

    def combine(b, c):
        pp_copy(b, c).wait_recv()
        for t in range(c + 1):
            comb[b, t] = part[b, core, t] + peer_part[b, t]

    def send_far(b, c):
        for t in range(1 if c == last else 0, c):
            far_copy(b, t).start()

    n_blocks = n_rows // ROWS
    toks = ROWS // heads

    def attend(b, keys):
        blocks = [slice(i * ROWS, (i + 1) * ROWS) for i in range(n_blocks)]
        scores = [dot(q_v[b, rows, :], kv[b, 0, 0:keys, :], NT) for rows in blocks]
        probs = []
        for i, rows in enumerate(blocks):
            lim = cap[i * toks:(i + 1) * toks, 0:keys]
            lim = jnp.broadcast_to(lim[:, None, :], (toks, heads, keys)).reshape(ROWS, keys)
            s = jnp.minimum(scores[i], lim)
            top = jnp.max(s, axis=-1, keepdims=True)
            e = jnp.exp2((s - top) * (scale * math.log2(math.e)))
            prob = e * (1.0 / jnp.sum(e, axis=-1, keepdims=True))
            p_low[rows, 0:keys] = prob.astype(jnp.bfloat16)
            probs.append((prob, prob.astype(jnp.bfloat16)))
        grads = []
        for rows, (prob, low) in zip(blocks, probs):
            g = g_v[b, rows, :]
            v = kv[b, 1, 0:keys, :]
            dp = dot(g, v, NT)
            o = dot(low, v).astype(jnp.bfloat16)
            o_v[b, rows, :] = o
            delta = jnp.sum(g.astype(jnp.float32) * o.astype(jnp.float32), axis=-1, keepdims=True)
            ds = (prob * (dp - delta)).astype(jnp.bfloat16)
            d_low[rows, 0:keys] = ds
            grads.append(ds)
        for rows, ds in zip(blocks, grads):
            dq_v[b, rows, :] = (dot(ds, kv[b, 0, 0:keys, :]) * scale).astype(jnp.bfloat16)

    def key_grads(b, keys):
        dv = dot(g_v[b], p_low[:, 0:keys], TN)
        dk = dot(q_v[b], d_low[:, 0:keys], TN)
        left = lax.broadcasted_iota(jnp.int32, (dim, LANE), 1) < piece
        for t in range(keys // LANE):
            cols = slice(t * LANE, (t + 1) * LANE)
            dk_t, dv_t = dk[:, cols], dv[:, cols]
            part[b, 0, t] = jnp.where(left, dk_t, pltpu.roll(dv_t, piece, 1))
            part[b, 1, t] = jnp.where(left, pltpu.roll(dk_t, piece, 1), dv_t)

    def per_chip(fn):
        for c in range(n_chip):
            @pl.when(chip == c)
            def _():
                fn(c)

    def out_copies(b):
        return (pltpu.make_async_copy(o_v.at[b], o_out.at[b], out_sem.at[0]),
                pltpu.make_async_copy(dq_v.at[b], dq_out.at[b], out_sem.at[1]))

    def step(b, _):
        @pl.when(b == 0)
        def _():
            send_own(2)

        q_copy(b).wait()
        g_copy(b).wait()
        per_chip(functools.partial(work, b))
        return 0

    def work(b, c):
        arrived(b, c)
        q_pos = rank * piece + lax.broadcasted_iota(jnp.int32, (piece, LANE), 0)
        for t in range(c + 1):
            k_pos = t * LANE + lax.broadcasted_iota(jnp.int32, (piece, LANE), 1)
            ids = jnp.broadcast_to(key_doc[b, :, t * LANE:(t + 1) * LANE], (piece, LANE))
            seen = (ids == qry_doc[b]) & (k_pos <= q_pos)
            cap[:, t * LANE:(t + 1) * LANE] = jnp.where(seen, POS_BIG, NEG_BIG)
        attend(b, (c + 1) * LANE)

        @pl.when(b + AHEAD < n_batch)
        def _():
            send_own(b + AHEAD)

        @pl.when(b > 0)
        def _():
            combine(b - 1, c)
            send_far(b - 1, c)

        if c > 0:
            @pl.when(b == 0)
            def _():
                forward(1, c)

            @pl.when(b + 2 < n_batch)
            def _():
                forward(b + 2, c)
        if c == last:
            @pl.when((b > 1) & (b <= LATE))
            def _():
                merge(b - 2)

            @pl.when(b >= LATE)
            def _():
                merge(b - 1)
        key_grads(b, (c + 1) * LANE)
        pp_copy(b, c).start()
        for copy in out_copies(b):
            copy.start()

    lax.fori_loop(0, n_batch, step, 0)

    def finish_loop(c):
        combine(n_batch - 1, c)
        send_far(n_batch - 1, c)
        if c == last:
            merge(n_batch - 1)

    per_chip(finish_loop)

    def finish(b, _):
        fin_acc = comb[b, chip]
        peer_part[b, 0] = fin_acc
        @pl.when((chip == 0) & over(b))
        def _():
            far_arrival(b, 1).wait_recv()
            relay_copy(b).start()
        for slot in range(last):
            used = slot < last - chip
            if slot == 1:
                used &= chip != 0

            @pl.when(used)
            def _():
                far_arrival(b, slot).wait_recv()
                peer_part[b, 0] += far_part[b, slot]
        total = peer_part[b, 0].T
        fin[b, 0] = (total[:piece] * scale).astype(jnp.bfloat16)
        fin[b, 1] = total[piece:].astype(jnp.bfloat16)
        pltpu.make_async_copy(fin.at[b, 0], dk_out.at[b], out_sem.at[2]).start()
        pltpu.make_async_copy(fin.at[b, 1], dv_out.at[b], out_sem.at[3]).start()
        return 0

    lax.fori_loop(0, n_batch, finish, 0)

    for to in range(n_grp):
        @pl.when(to > rank)
        def _():
            doc_copy(to).wait_send()

    def sent(src, sem):
        remote(src, src, sem, kv_recv.at[0, 0], peer).wait_send()

    own_all = kv.at[:, :, at(rank), :]

    @pl.when(core == 0)
    def _():
        sent(own_all, kv_send.at[chip])
    for far in range(1, n_chip):
        @pl.when(far > chip)
        def _():
            sent(own_all, kv_send.at[far])
    for t in range(last):
        @pl.when(t < chip)
        def _():
            sent(own_all, fwd_send.at[t])
            sent(comb.at[:, t], far_send.at[t])

    @pl.when(chip == 0)
    def _():
        sent(comb.at[0:n_batch // 2 - 1, 0], far_send.at[1])
    per_chip(lambda c: sent(part.at[:, 0, 0:c + 1], pp_send.at[0]))
    pltpu.make_async_copy(o_v, o_out, out_sem.at[0]).wait()
    pltpu.make_async_copy(dq_v, dq_out, out_sem.at[1]).wait()
    pltpu.make_async_copy(fin.at[:, 0], dk_out, out_sem.at[2]).wait()
    pltpu.make_async_copy(fin.at[:, 1], dv_out, out_sem.at[3]).wait()


def write_out(*refs):
    n = (len(refs) - 1) // 2
    copies = [pltpu.make_async_copy(refs[i], refs[n + i], refs[-1].at[i]) for i in range(n)]
    for copy in copies:
        copy.start()
    for copy in copies:
        copy.wait()


def solution(mesh):
    n_grp = mesh.shape['cp']
    n_chip = n_grp // CORES
    seq_spec = P('dp', 'cp', None, None)
    id_spec = P('dp', 'cp')

    def per_device(query, keys, values, grad_out, doc_id):
        n_batch, piece, heads, dim = query.shape
        n_rows = piece * heads
        n_keys = n_grp * piece
        flat = (n_batch, n_rows, dim)
        small = (n_batch, piece, dim)
        bf16, f32, i32 = jnp.bfloat16, jnp.float32, jnp.int32
        any_spec = pl.BlockSpec(memory_space=pl.ANY)
        dma = pltpu.SemaphoreType.DMA
        tile = (dim, LANE)
        outs = pl.pallas_call(
            functools.partial(kernel, n_grp, heads),
            out_shape=[jax.ShapeDtypeStruct(flat, bf16), jax.ShapeDtypeStruct(flat, bf16),
                       jax.ShapeDtypeStruct(small, bf16), jax.ShapeDtypeStruct(small, bf16)],
            in_specs=[any_spec] * 5,
            out_specs=[any_spec] * 4,
            scratch_shapes=[
                pltpu.VMEM(flat, bf16), pltpu.VMEM(flat, bf16),
                pltpu.VMEM(flat, bf16), pltpu.VMEM(flat, bf16),
                pltpu.VMEM((n_batch, 2, n_keys, dim), bf16),
                pltpu.VMEM((n_batch, piece), i32),
                pltpu.VMEM((n_grp, n_batch, LANE), i32),
                pltpu.VMEM((n_batch, 1, n_keys), i32),
                pltpu.VMEM((n_batch, piece, LANE), i32),
                pltpu.VMEM((piece, n_keys), f32),
                pltpu.VMEM((n_rows, n_keys), bf16), pltpu.VMEM((n_rows, n_keys), bf16),
                pltpu.VMEM((n_batch, 2, n_chip) + tile, f32),
                pltpu.VMEM((n_batch, n_chip) + tile, f32),
                pltpu.VMEM((n_batch, n_chip) + tile, f32),
                pltpu.VMEM((n_batch, n_chip - 1) + tile, f32),
                pltpu.VMEM((n_batch, 2, piece, dim), bf16),
                dma((3,)), dma((n_batch, 2)), dma((n_grp,)), dma((n_grp,)),
                dma((n_chip,)), dma((n_batch, n_chip)),
                dma((n_chip - 1,)), dma((n_batch,)),
                dma((1,)), dma((n_batch,)),
                dma((n_chip - 1,)), dma((n_batch, n_chip - 1)),
                dma((4,)),
            ],
            compiler_params=pltpu.CompilerParams(
                collective_id=0, has_side_effects=True, vmem_limit_bytes=48 * 2**20),
            name='mqa',
        )(query.reshape(flat), grad_out.reshape(flat), *[pltpu.with_memory_space_constraint(a, pltpu.HBM) for a in
            (keys.reshape(small), values.reshape(small), doc_id)])
        attn_out, grad_query, grad_keys, grad_values = pl.pallas_call(
            write_out,
            out_shape=[jax.ShapeDtypeStruct(a.shape, a.dtype) for a in outs],
            in_specs=[any_spec] * 4,
            out_specs=[pl.BlockSpec(memory_space=pltpu.HBM)] * 4,
            scratch_shapes=[dma((4,))],
            compiler_params=pltpu.CompilerParams(vmem_limit_bytes=2**20),
            name='write',
        )(*outs)
        return (attn_out.reshape(query.shape), grad_query.reshape(query.shape),
                grad_keys.reshape(keys.shape), grad_values.reshape(values.shape))

    return jax.shard_map(per_device, mesh=mesh,
                         in_specs=(seq_spec, seq_spec, seq_spec, seq_spec, id_spec),
                         out_specs=(seq_spec, seq_spec, seq_spec, seq_spec), check_vma=False)
```
